32 devices in a mesh: dp: 4 (over x, core), ctx: 8 (over z, y).
Axes of the slice: x: 2, y: 2, z: 4, core: 2. Of those that a mesh axis runs over, the one named last changes fastest.
Arguments:
- inputs: bfloat16 [8, 512, 2048], P('dp', 'ctx'), may hold values from -6 to 6
- cotangent: bfloat16 [8, 512, 2048], P('dp', 'ctx'), may hold values from -6 to 6
- lengths: int32 [8], P('dp'), may hold values from 128 to 512, as said below
- query_weight: bfloat16 [2048, 2048], P(('dp', 'ctx')), may hold values from -0.125 to 0.125
- key_weight: bfloat16 [2048, 2048], P(('dp', 'ctx')), may hold values from -0.125 to 0.125
- value_weight: bfloat16 [2048, 2048], P(('dp', 'ctx')), may hold values from -0.125 to 0.125
- mix_weight: bfloat16 [2048, 2048], P(('dp', 'ctx')), may hold values from -0.75 to 0.75
- gate_weight: bfloat16 [2048, 8192], P(('dp', 'ctx')), may hold values from -0.125 to 0.125
- up_weight: bfloat16 [2048, 8192], P(('dp', 'ctx')), may hold values from -0.125 to 0.125
- down_weight: bfloat16 [2048, 8192], P(('dp', 'ctx')), may hold values from -0.0625 to 0.0625
- attn_gain: bfloat16 [2048], P(('dp', 'ctx')), may hold values from 0.5 to 1.5
- ffn_gain: bfloat16 [2048], P(('dp', 'ctx')), may hold values from 0.5 to 1.5
Outputs:
- activations: bfloat16 [8, 512, 2048], P('dp', 'ctx')
- input_grad: bfloat16 [8, 512, 2048], P('dp', 'ctx')
- query_grad: float32 [2048, 2048], P(('dp', 'ctx'))
- key_grad: float32 [2048, 2048], P(('dp', 'ctx'))
- value_grad: float32 [2048, 2048], P(('dp', 'ctx'))
- mix_grad: float32 [2048, 2048], P(('dp', 'ctx'))
- gate_grad: float32 [2048, 8192], P(('dp', 'ctx'))
- up_grad: float32 [2048, 8192], P(('dp', 'ctx'))
- down_grad: float32 [2048, 8192], P(('dp', 'ctx'))
- attn_gain_grad: float32 [2048], P(('dp', 'ctx'))
- ffn_gain_grad: float32 [2048], P(('dp', 'ctx'))
The draws below stay inside these ranges and needn't reach their ends.
Inputs may be any that keep to these rules, and one draw needn't show every extreme that they name: `lengths`: each sequence has 128 to 512 valid slots at its start; the first sequence is full.
All inputs are finite; a program needn't handle non-finite values.
Results may differ from the reference program's by a relative error of at most 0.03.
Values may be sent and summed in bfloat16 or wider, within the bound.
No kernel may reach another device: no remote copies, remote signals or barrier semaphores. Data moves between devices by JAX's collectives and lax.ppermute only.
A program may use at most 576 MiB of HBM per device.

```python
import jax
import jax.numpy as jnp
from jax import lax

D = 2048
HEADS = 32
FF = 8192
SEQ = 512
BATCH = 8


def draw_lengths(key, part):
    drawn = jax.random.randint(key, (BATCH,), SEQ // 4, SEQ + 1).astype(jnp.int32)
    return drawn.at[0].set(SEQ)


def spiked(values, stream_key, source, target, parts, factor):
    owner, partner = [(jnp.arange(values.shape[axis_at]) // (values.shape[axis_at] // parts)).reshape([-1 if axis == axis_at else 1 for axis in range(values.ndim)]) for axis_at in (source, target)]
    chosen = jax.random.permutation(stream_key, parts)[partner]
    strong = (owner == chosen) | (owner == (partner + parts // 2) % parts)
    return jnp.where(strong, factor * values, values)


def levels(stream_key, extent, shards, smallest, top_value):
    def one(position, shards_of):
        heights = jax.random.uniform(jax.random.fold_in(jax.random.fold_in(stream_key, 6), position), (shards_of,), jnp.float32, smallest / len(shards), top_value / len(shards))
        return jnp.repeat(jnp.exp(heights), extent[position] // shards_of).reshape((-1,) + (1,) * (len(extent) - position - 1))

    loudness = one(*shards[0])
    for cut in shards[1:]:
        loudness = loudness * one(*cut)
    return loudness


def scatter_about(key, dims, deviation, limit, cuts=(), kind=jnp.bfloat16):
    gain = levels(key, dims, cuts, -0.22, 0.18) if cuts else 1.0
    values = jax.random.normal(key, dims, jnp.float32) * deviation * gain
    return jnp.minimum(jnp.maximum(values, -limit), limit).astype(kind)


def gaussian_with(rng, shape, scale, bound, split, heavy, kind=jnp.bfloat16):
    entries = scale * jax.random.normal(rng, shape, jnp.float32)
    if split:
        entries = entries * levels(rng, shape, split, -0.22, 0.18)
    return jnp.clip(spiked(entries, jax.random.fold_in(rng, 3), *heavy), -bound, bound).astype(kind)


def setup_inputs(seed: int = 0) -> dict:
    key_of = jax.random.split(jax.random.key(seed), 13)
    inputs = gaussian_with(key_of[0], (BATCH, SEQ, D), 1.0, 6.0, ((0, 4), (1, 8)), (1, 2, 8, 2.0))
    cotangent = gaussian_with(key_of[1], (BATCH, SEQ, D), 1.0, 6.0, ((0, 4), (1, 8)), (1, 2, 8, 2.0))
    lengths = draw_lengths(jax.random.fold_in(key_of[12], 71), 0)
    query_weight = scatter_about(key_of[3], (D, D), D ** -0.5, 0.125, ((0, 32),))
    key_weight = scatter_about(key_of[4], (D, D), D ** -0.5, 0.125, ((0, 32),))
    value_weight = scatter_about(key_of[5], (D, D), D ** -0.5, 0.125, ((0, 32),))
    mix_weight = scatter_about(key_of[6], (D, D), (max(D * 16 // SEQ, 1)) ** -0.5, 0.75, ((0, 32),))
    gate_weight = scatter_about(key_of[7], (D, FF), D ** -0.5, 0.125, ((0, 32),))
    up_weight = scatter_about(key_of[8], (D, FF), D ** -0.5, 0.125, ((0, 32),))
    down_weight = scatter_about(key_of[9], (D, FF), FF ** -0.5, 0.0625, ((0, 32),))
    attn_gain = jnp.clip(1.0 + 0.1 * jax.random.normal(key_of[10], (D,), jnp.float32), 0.5, 1.5).astype(jnp.bfloat16)
    ffn_gain = jnp.clip(1.0 + 0.1 * jax.random.normal(key_of[11], (D,), jnp.float32), 0.5, 1.5).astype(jnp.bfloat16)
    return {"inputs": inputs, "cotangent": cotangent, "lengths": lengths, "query_weight": query_weight, "key_weight": key_weight, "value_weight": value_weight, "mix_weight": mix_weight, "gate_weight": gate_weight, "up_weight": up_weight, "down_weight": down_weight, "attn_gain": attn_gain, "ffn_gain": ffn_gain}


EPSILON = 1e-05
THETA = 130000.0
NEGATIVE = -1e+30
HIGHEST = lax.Precision.HIGHEST

@jax.custom_vjp
def low(v):
    return lax.optimization_barrier(v.astype(jnp.bfloat16)).astype(jnp.float32)

@jax.custom_vjp
def low_back(v):
    return v

def low_keep(v):
    return (low(v), None)

def low_pass(kept, grad):
    return (grad,)

def back_keep(v):
    return (v, None)

def back_low(kept, grad):
    return (low(grad),)
low.defvjp(low_keep, low_pass)
low_back.defvjp(back_keep, back_low)

def rotation(positions, half):
    freqs = THETA ** (-(jnp.arange(half, dtype=jnp.float32) * 2.0) / (2.0 * half))
    angles = positions.astype(jnp.float32)[:, None] * freqs[None, :]
    return (jnp.cos(angles), jnp.sin(angles))

def rotate(tensor, cosine, sine):
    half = tensor.shape[-1] // 2
    first = tensor[..., :half]
    second = tensor[..., half:]
    cosine = cosine[:, None, :]
    sine = sine[:, None, :]
    return jnp.concatenate([first * cosine - second * sine, second * cosine + first * sine], axis=-1)

def normalize(values):
    factor = lax.rsqrt(lax.optimization_barrier(jnp.mean(values * values, axis=-1, keepdims=True)) + EPSILON)
    return values * factor

def matmul(left, right):
    return jnp.dot(left, right, precision=HIGHEST)

def reference(inputs, cotangent, lengths, query_weight, key_weight, value_weight, mix_weight, gate_weight, up_weight, down_weight, attn_gain, ffn_gain):
    batch, seq, width = inputs.shape
    head_size = width // HEADS
    scale = head_size ** (-0.5)
    positions = jnp.arange(seq, dtype=jnp.int32)
    cosine, sine = rotation(positions, head_size // 2)
    block = min(512, seq)

    def layer(params, values, length):
        w_query, w_key, w_value, w_mix, w_gate, w_up, w_down, gain_one, gain_two = params
        xn_one = low(normalize(values) * gain_one)
        queries = low_back(matmul(xn_one, w_query)).reshape(seq, HEADS, head_size)
        keys = low_back(matmul(xn_one, w_key)).reshape(seq, HEADS, head_size)
        vals = low(low_back(matmul(xn_one, w_value))).reshape(seq, HEADS, head_size)
        query_rot = low(rotate(queries, cosine, sine))
        key_rot = low(rotate(keys, cosine, sine))

        def attend(args):
            query_block, start = args
            query_pos = start + jnp.arange(block, dtype=jnp.int32)
            scores = low_back(jnp.einsum('qhd,khd->hqk', query_block, key_rot, precision=HIGHEST)) * scale
            allowed = (positions[None, :] <= query_pos[:, None]) & (positions[None, :] < length)
            masked = jnp.where(allowed[None], scores, NEGATIVE)
            peak = lax.optimization_barrier(jnp.max(masked, axis=-1, keepdims=True))
            expo = jnp.where(allowed[None], jnp.exp(masked - peak), 0.0)
            prob = expo / lax.optimization_barrier(jnp.sum(expo, axis=-1, keepdims=True))
            return jnp.einsum('hqk,khd->qhd', low(prob), vals, precision=HIGHEST)
        blocks = query_rot.reshape(seq // block, block, HEADS, head_size)
        starts = jnp.arange(seq // block, dtype=jnp.int32) * block
        attended = lax.map(jax.checkpoint(attend), (blocks, starts)).reshape(seq, width)
        mixed_in = low(low_back(attended))
        residual = values + low_back(matmul(mixed_in, w_mix))
        xn_two = low(normalize(residual) * gain_two)
        gate = low_back(matmul(xn_two, w_gate))
        up = low_back(matmul(xn_two, w_up))
        hidden = low(jax.nn.silu(gate) * up)
        branch = jnp.dot(hidden, w_down.T, precision=HIGHEST)
        valid = (positions < length).astype(jnp.float32)[:, None]
        return valid * (residual + branch)

    def forward(params, values):

        def one(args):
            return layer(params, args[0], args[1])
        return lax.map(jax.checkpoint(one), (values, lengths))
    params = tuple((w.astype(jnp.float32) for w in (query_weight, key_weight, value_weight, mix_weight, gate_weight, up_weight, down_weight, attn_gain, ffn_gain)))
    result, pullback = jax.vjp(forward, params, inputs.astype(jnp.float32))
    param_grads, input_grad = pullback(cotangent.astype(jnp.float32))
    return (result.astype(jnp.bfloat16), input_grad.astype(jnp.bfloat16), param_grads[0], param_grads[1], param_grads[2], param_grads[3], param_grads[4], param_grads[5], param_grads[6], param_grads[7], param_grads[8])
```

```python
import functools

import jax
import jax.numpy as jnp
from jax import lax
from jax.experimental import pallas as pl
from jax.experimental.pallas import tpu as pltpu
from jax.sharding import PartitionSpec as P

HEADS = 32
EPSILON = 1e-05
THETA = 130000.0
NEGATIVE = -1e30
QUERY_ROWS = 512
BF16 = jnp.bfloat16
F32 = jnp.float32


def normalize(values):
    factor = lax.rsqrt(jnp.mean(values * values, axis=-1, keepdims=True) + EPSILON)
    return (values * factor, factor)


def contract(left, right, left_dim, right_dim):
    return lax.dot_general(
        left, right, (((left_dim,), (right_dim,)), ((), ())), preferred_element_type=F32
    )


class Ring:
    def __init__(self, size):
        self.size = size
        self.order = list(range(0, size, 2)) + list(range(size - 1, 0, -2))
        places = [self.order.index(i) for i in range(size)]
        self.place = jnp.array(places, jnp.int32)[lax.axis_index("ctx")]
        self.table = jnp.array(self.order, jnp.int32)

    def owner(self, ahead):
        return self.table[lax.rem(self.place + ahead + self.size, self.size)]

    def owners(self):
        return jnp.roll(jnp.concatenate([self.table, self.table]), -self.place)[: self.size]

    def shift(self, value, by):
        pairs = [
            (self.order[i], self.order[(i + by) % self.size]) for i in range(self.size)
        ]
        return lax.ppermute(value, "ctx", pairs)

    def gather(self, value):
        size, half = self.size, self.size // 2
        pieces = [None] * size
        pieces[0] = value
        right = left = value
        for step in range(1, half):
            right = self.shift(right, 1)
            left = self.shift(left, -1)
            pieces[size - step] = right
            pieces[step] = left
        rows = value.shape[0] // 2
        pieces[half] = jnp.concatenate(
            [self.shift(right[:rows], 1), self.shift(left[rows:], -1)], axis=0
        )
        return pieces

    def scatter_sum(self, part):
        size, half = self.size, self.size // 2
        lower, upper, whole = 0, 1, 2
        right = part(half, lower).astype(BF16)
        left = part(half, upper).astype(BF16)
        right = self.shift(right, 1)
        left = self.shift(left, -1)
        for step in range(1, half):
            if step == 1:
                right = jnp.concatenate(
                    [part(half - 1, lower) + right.astype(F32), part(half - 1, upper)], axis=1
                )
                left = jnp.concatenate(
                    [part(half + 1, lower), part(half + 1, upper) + left.astype(F32)], axis=1
                )
            else:
                right = part(half - step, whole) + right.astype(F32)
                left = part(half + step, whole) + left.astype(F32)
            right = self.shift(right.astype(BF16), 1)
            left = self.shift(left.astype(BF16), -1)
        if half == 1:
            return jnp.concatenate(
                [part(0, lower) + right.astype(F32), part(0, upper) + left.astype(F32)], axis=1
            )
        return part(0, whole) + right.astype(F32) + left.astype(F32)

    def exchange(self, pieces):
        size = self.size
        out = [None] * size
        out[0] = pieces[0]
        for by in range(1, size):
            out[size - by] = self.shift(pieces[by], by)
        return out

    def place_in_order(self, pieces):
        out = jnp.zeros((self.size,) + pieces[0].shape, pieces[0].dtype)
        for ahead in range(self.size):
            out = lax.dynamic_update_index_in_dim(out, pieces[ahead], self.owner(ahead), 0)
        return out

    def take_relative(self, stacked):
        return [
            lax.dynamic_index_in_dim(stacked, self.owner(ahead), 0, keepdims=False)
            for ahead in range(self.size)
        ]


def column_blocks(weight, size):
    width = weight.shape[1] // size
    return jnp.stack([weight[:, i * width : (i + 1) * width] for i in range(size)])


def join_columns(stacked):
    return jnp.concatenate([stacked[i] for i in range(stacked.shape[0])], axis=1)


def swap_halves(values, half):
    width = values.shape[-1]
    if width == 2 * half:
        return jnp.concatenate([values[:, half:], values[:, :half]], axis=1)
    lane = lax.broadcasted_iota(jnp.int32, values.shape, 1)
    ahead = pltpu.roll(values, width - half, 1)
    behind = pltpu.roll(values, half, 1)
    return jnp.where(lax.rem(lane, 2 * half) < half, ahead, behind)


def head_only(values, lane, head, head_size):
    inside = (lane >= head * head_size) & (lane < (head + 1) * head_size)
    return jnp.where(inside, values, jnp.zeros_like(values))


def flat(ref):
    value = ref[...]
    return value.reshape((value.shape[0] * value.shape[1], value.shape[2]))


def forward_kernel(
    head_size, lengths_ref, q_ref, k_ref, v_ref, cq_ref, sq_ref, ck_ref, sk_ref, qp_ref, kp_ref,
    out_ref, qr_ref, kr_ref, vr_ref, lse_ref,
):
    length = lengths_ref[pl.program_id(0)]
    half = head_size // 2
    queries = flat(q_ref)
    keys = flat(k_ref)
    queries = (queries * cq_ref[...] + swap_halves(queries, half) * sq_ref[...]).astype(BF16)
    keys = (keys * ck_ref[...] + swap_halves(keys, half) * sk_ref[...]).astype(BF16)
    values = flat(v_ref).astype(BF16)
    qr_ref[...] = queries.reshape(qr_ref.shape)
    kr_ref[...] = keys.reshape(kr_ref.shape)
    vr_ref[...] = values.reshape(vr_ref.shape)
    rows, width = queries.shape
    lane = lax.broadcasted_iota(jnp.int32, (rows, width), 1)
    query_pos = qp_ref[:, 0:1]
    key_pos = kp_ref[0:1, :]
    allowed = (key_pos <= query_pos) & (key_pos < length)
    total = jnp.zeros((rows, width), F32)
    scale = head_size ** (-0.5)
    for head in range(width // head_size):
        one = head_only(queries, lane, head, head_size)
        scores = contract(one, keys, 1, 1) * scale
        masked = jnp.where(allowed, scores, NEGATIVE)
        peak = jnp.max(masked, axis=-1, keepdims=True)
        weights = jnp.where(allowed, jnp.exp(masked - peak), 0.0)
        mass = jnp.sum(weights, axis=-1, keepdims=True)
        lse_ref[:, head : head + 1] = peak + jnp.log(mass)
        mixed = contract(weights.astype(BF16), values, 1, 0) / mass
        total = total + head_only(mixed, lane, head, head_size)
    out_ref[...] = total.astype(BF16).reshape(out_ref.shape)


def backward_kernel(
    head_size, lengths_ref, q_ref, k_ref, v_ref, g_ref, lse_ref, cq_ref, sq_ref, ck_ref, sk_ref, qp_ref,
    kp_ref, dq_ref, dk_ref, dv_ref, dk_sum, dv_sum,
):
    length = lengths_ref[pl.program_id(0)]
    half = head_size // 2
    queries, keys, values, grads = flat(q_ref), flat(k_ref), flat(v_ref), flat(g_ref)
    rows, width = queries.shape
    lane = lax.broadcasted_iota(jnp.int32, (rows, width), 1)
    allowed = (kp_ref[0:1, :] <= qp_ref[:, 0:1]) & (kp_ref[0:1, :] < length)
    scale = head_size ** (-0.5)

    @pl.when(pl.program_id(1) == 0)
    def start():
        dk_sum[...] = jnp.zeros_like(dk_sum)
        dv_sum[...] = jnp.zeros_like(dv_sum)

    dq = jnp.zeros((rows, width), F32)
    for head in range(width // head_size):
        one = head_only(queries, lane, head, head_size)
        grad = head_only(grads, lane, head, head_size)
        scores = contract(one, keys, 1, 1) * scale
        prob = jnp.where(
            allowed,
            jnp.exp(jnp.where(allowed, scores, NEGATIVE) - lse_ref[:, head : head + 1]),
            0.0,
        )
        grad_prob = contract(grad, values, 1, 1)
        delta = jnp.sum(prob * grad_prob, axis=-1, keepdims=True)
        grad_score = (prob * (grad_prob - delta) * scale).astype(BF16)
        dq = dq + head_only(contract(grad_score, keys, 1, 0), lane, head, head_size)
        dk_sum[...] += contract(grad_score, one, 0, 0)
        dv_sum[...] += contract(prob.astype(BF16), grad, 0, 0)
    dq = dq * cq_ref[...] - swap_halves(dq, half) * sq_ref[...]
    dq_ref[...] = dq.astype(BF16).reshape(dq_ref.shape)

    @pl.when(pl.program_id(1) == pl.num_programs(1) - 1)
    def finish():
        dk = dk_sum[...]
        dk = dk * ck_ref[...] - swap_halves(dk, half) * sk_ref[...]
        dk_ref[...] = dk.astype(BF16).reshape(dk_ref.shape)
        dv_ref[...] = dv_sum[...].astype(BF16).reshape(dv_ref.shape)


class Attention:
    def __init__(self, size, groups, slots, width, head_size, lengths, owners):
        self.size, self.groups, self.slots, self.width = size, groups, slots, width
        self.head_size = head_size
        self.lengths = lengths
        self.heads = width // head_size
        self.steps = max(1, min(size, QUERY_ROWS // slots))
        half = head_size // 2
        positions = (owners[:, None] * slots + jnp.arange(slots, dtype=jnp.int32)[None]).reshape(-1)
        freqs = THETA ** (-(jnp.arange(half, dtype=F32) * 2.0) / (2.0 * half))
        angles = positions.astype(F32)[:, None] * freqs[None, :]
        cosine, sine = jnp.cos(angles), jnp.sin(angles)
        self.cosine = jnp.tile(cosine, (1, 2 * self.heads))
        self.sine = jnp.tile(jnp.concatenate([-sine, sine], axis=1), (1, self.heads))
        self.query_pos = jnp.broadcast_to(positions[:, None], (positions.shape[0], 128))
        self.key_pos = jnp.broadcast_to(positions[None, :], (8, positions.shape[0]))
        total = size * slots
        rows = self.steps * slots
        self.grid = (groups, size // self.steps)
        self.q_spec = self.tokens(self.steps, width, 0, True)
        self.k_spec = self.tokens(size, width, 0, False)
        self.table_q = pl.BlockSpec((rows, width), lambda b, i, *_: (i, 0))
        self.table_k = pl.BlockSpec((total, width), lambda b, i, *_: (0, 0))
        self.pos_q = pl.BlockSpec((rows, 128), lambda b, i, *_: (i, 0))
        self.pos_k = pl.BlockSpec((8, total), lambda b, i, *_: (0, 0))
        self.lse = pl.BlockSpec((None, rows, self.heads), lambda b, i, *_: (b, i, 0))
        self.lse_shape = jax.ShapeDtypeStruct((groups, total, self.heads), F32)
        self.shape = jax.ShapeDtypeStruct((size, groups, slots, width), BF16)
        self.work = groups * self.heads * total * total

    def tokens(self, count, width, column, moving):
        return pl.BlockSpec(
            (count, None, self.slots, width),
            (lambda b, i, *_: (i, b, 0, column)) if moving else (lambda b, i, *_: (0, b, 0, column)),
        )

    def split(self, array):
        return array.reshape(self.size, self.groups, self.slots, -1)

    def cost(self, matmuls):
        return pl.CostEstimate(
            flops=2 * matmuls * self.work * self.head_size,
            transcendentals=self.work,
            bytes_accessed=8 * self.size * self.groups * self.slots * self.width * 2,
        )

    def forward(self, projected):
        width = self.width
        if width % 128 == 0:
            arrays = (self.split(projected),) * 3
            columns = (0, 1, 2)
        else:
            arrays = tuple(
                self.split(projected[:, i * width : (i + 1) * width]) for i in range(3)
            )
            columns = (0, 0, 0)
        return pl.pallas_call(
            functools.partial(forward_kernel, self.head_size),
            grid_spec=pltpu.PrefetchScalarGridSpec(
                num_scalar_prefetch=1,
                grid=self.grid,
                in_specs=[
                    self.tokens(self.steps, width, columns[0], True),
                    self.tokens(self.size, width, columns[1], False),
                    self.tokens(self.size, width, columns[2], False),
                    self.table_q, self.table_q, self.table_k, self.table_k, self.pos_q, self.pos_k,
                ],
                out_specs=[self.q_spec, self.q_spec, self.k_spec, self.k_spec, self.lse],
            ),
            out_shape=[self.shape] * 4 + [self.lse_shape],
            cost_estimate=self.cost(2),
            name="attention_forward",
        )(
            self.lengths, *arrays, self.cosine, self.sine, self.cosine, self.sine, self.query_pos, self.key_pos
        )

    def backward(self, queries, keys, values, grads, lse):
        total = self.size * self.slots
        return pl.pallas_call(
            functools.partial(backward_kernel, self.head_size),
            grid_spec=pltpu.PrefetchScalarGridSpec(
                num_scalar_prefetch=1,
                grid=self.grid,
                in_specs=[
                    self.q_spec, self.k_spec, self.k_spec, self.q_spec, self.lse,
                    self.table_q, self.table_q, self.table_k, self.table_k, self.pos_q, self.pos_k,
                ],
                out_specs=[self.q_spec, self.k_spec, self.k_spec],
                scratch_shapes=[pltpu.VMEM((total, self.width), F32)] * 2,
            ),
            out_shape=[self.shape] * 3,
            cost_estimate=self.cost(5),
            name="attention_backward",
        )(
            self.lengths, queries, keys, values, self.split(grads), lse,
            self.cosine, self.sine, self.cosine, self.sine, self.query_pos, self.key_pos,
        )


def body(
    inputs, cotangent, lengths, query_weight, key_weight, value_weight, mix_weight, gate_weight,
    up_weight, down_weight, attn_gain, ffn_gain,
):
    groups, slots, width = inputs.shape
    head_size = width // HEADS
    size = lax.axis_size("ctx")
    shares = lax.axis_size("dp")
    rows = groups * slots
    ring = Ring(size)
    owners = ring.owners()
    local = width // size
    hidden_local = gate_weight.shape[1] // size
    gain_one = attn_gain.astype(F32)[:, None]
    gain_two = ffn_gain.astype(F32)[:, None]

    def over_shares(value):
        return lax.all_gather(value, "dp", axis=0, tiled=True)

    def scaled(weight, gain):
        return (weight.astype(F32) * gain).astype(BF16)

    def to_columns(weights):
        blocks = jnp.concatenate([column_blocks(w, size) for w in weights], axis=2)
        got = ring.place_in_order(ring.exchange(ring.take_relative(blocks)))
        return got.reshape(-1, got.shape[2])

    attn_rows = to_columns([scaled(w, gain_one) for w in (query_weight, key_weight, value_weight)])
    attn_columns = over_shares(attn_rows)
    ffn_rows = to_columns(
        [scaled(gate_weight, gain_two), scaled(up_weight, gain_two), down_weight]
    )
    gate_columns = over_shares(ffn_rows[:, :hidden_local])
    up_columns = over_shares(ffn_rows[:, hidden_local : 2 * hidden_local])
    down_columns = over_shares(ffn_rows[:, 2 * hidden_local :])
    mix_full = lax.all_gather(mix_weight, ("dp", "ctx"), axis=0, tiled=True)

    block_in = inputs.reshape(rows, width).astype(F32)
    positions = lax.axis_index("ctx") * slots + jnp.arange(slots, dtype=jnp.int32)
    valid = (positions[None, :] < lengths[:, None]).astype(F32).reshape(rows, 1)
    normed_one, factor_one = normalize(block_in)
    one_all = jnp.concatenate(ring.gather(normed_one.astype(BF16)), axis=0)
    grad_out = cotangent.reshape(rows, width).astype(F32) * valid
    grad_all = jnp.concatenate(ring.gather(grad_out.astype(BF16)), axis=0)
    projected = contract(one_all, attn_columns, 1, 0)
    attention = Attention(size, groups, slots, local, head_size, lengths, owners)
    mixed, query_rot, key_rot, value_low, lse = attention.forward(projected)
    mixed_rows = mixed.reshape(size, rows, local)
    attended = join_columns(
        ring.place_in_order(ring.exchange([mixed_rows[r] for r in range(size)]))
    )
    residual = block_in + contract(attended, mix_full, 1, 0)

    normed_two, factor_two = normalize(residual)
    two_all = jnp.concatenate(ring.gather(normed_two.astype(BF16)), axis=0)
    gate = contract(two_all, gate_columns, 1, 0)
    up = contract(two_all, up_columns, 1, 0)
    sigma = jax.nn.sigmoid(gate)
    silu_gate = gate * sigma
    hidden = (silu_gate * up).astype(BF16)

    grad_hidden = contract(grad_all, down_columns, 1, 0)
    gate_low = (grad_hidden * up * sigma * (1.0 + gate * (1.0 - sigma))).astype(BF16)
    up_low = (grad_hidden * silu_gate).astype(BF16)

    def terms(values):
        half = width // 2

        def part(ahead, columns):
            chunk = values[ahead * rows : (ahead + 1) * rows]
            return (chunk[:, :half], chunk[:, half:], chunk)[columns]

        return part

    scaled_two = ring.scatter_sum(
        terms(contract(gate_low, gate_columns, 1, 1) + contract(up_low, up_columns, 1, 1))
    )
    dres = grad_out + factor_two * (
        scaled_two - normed_two * jnp.mean(normed_two * scaled_two, axis=-1, keepdims=True)
    )
    dres_low = dres.astype(BF16)
    branch = ring.scatter_sum(terms(contract(hidden, down_columns, 1, 1)))
    activations = (valid * (residual + branch)).astype(BF16)

    grad_mixed = contract(dres_low, mix_full, 1, 1).astype(BF16)
    grad_heads = jnp.concatenate(
        ring.exchange(ring.take_relative(column_blocks(grad_mixed, size))), axis=0
    )
    dres_all = jnp.concatenate(ring.gather(dres_low), axis=0)
    dq, dk, dv = attention.backward(query_rot, key_rot, value_low, grad_heads, lse)
    projected_grad = jnp.concatenate(
        [d.reshape(size * rows, local) for d in (dq, dk, dv)], axis=1
    )
    scaled_one = ring.scatter_sum(terms(contract(projected_grad, attn_columns, 1, 1)))
    input_grad = dres + factor_one * (
        scaled_one - normed_one * jnp.mean(normed_one * scaled_one, axis=-1, keepdims=True)
    )

    def to_rows(gradient):
        summed = lax.psum_scatter(gradient.astype(BF16), "dp", scatter_dimension=0, tiled=True)
        stacked = summed.reshape(size, summed.shape[0] // size, summed.shape[1])
        return ring.place_in_order(ring.exchange(ring.take_relative(stacked)))

    down_grad = join_columns(to_rows(contract(grad_all, hidden, 0, 0))).astype(F32)
    gate_raw = join_columns(to_rows(contract(two_all, gate_low, 0, 0))).astype(F32)
    up_raw = join_columns(to_rows(contract(two_all, up_low, 0, 0))).astype(F32)
    attn_raw = to_rows(contract(one_all, projected_grad, 0, 0))
    query_raw, key_raw, value_raw = (
        join_columns(attn_raw[:, :, i * local : (i + 1) * local]).astype(F32) for i in range(3)
    )
    mix_part = lax.psum_scatter(
        contract(mixed.reshape(size * rows, local), dres_all, 0, 0).astype(BF16),
        "dp",
        scatter_dimension=0,
        tiled=True,
    )
    mix_grad = lax.ppermute(
        mix_part,
        ("dp", "ctx"),
        [(i * size + j, j * shares + i) for i in range(shares) for j in range(size)],
    ).astype(F32)

    def row_sum(*pairs):
        return sum(jnp.sum(w.astype(F32) * g, axis=1) for w, g in pairs)

    attn_gain_grad = row_sum(
        (query_weight, query_raw), (key_weight, key_raw), (value_weight, value_raw)
    )
    ffn_gain_grad = row_sum((gate_weight, gate_raw), (up_weight, up_raw))
    return (
        activations.reshape(groups, slots, width),
        input_grad.astype(BF16).reshape(groups, slots, width),
        query_raw * gain_one,
        key_raw * gain_one,
        value_raw * gain_one,
        mix_grad,
        gate_raw * gain_two,
        up_raw * gain_two,
        down_grad,
        attn_gain_grad,
        ffn_gain_grad,
    )


def solution(mesh):
    rows = P(("dp", "ctx"), None)
    tokens = P("dp", "ctx", None)
    gains = P(("dp", "ctx"))
    return jax.shard_map(
        body,
        mesh=mesh,
        in_specs=(tokens, tokens, P("dp")) + (rows,) * 7 + (gains, gains),
        out_specs=(tokens, tokens) + (rows,) * 7 + (gains, gains),
        check_vma=False,
    )
```

```python
import functools

import jax
import jax.numpy as jnp
from jax import lax
from jax.experimental import pallas as pl
from jax.experimental.pallas import tpu as pltpu
from jax.sharding import PartitionSpec as P

HEADS = 32
EPSILON = 1e-05
THETA = 130000.0
NEGATIVE = -1e30
QUERY_ROWS = 512
BF16 = jnp.bfloat16
F32 = jnp.float32


def normalize(values):
    factor = lax.rsqrt(jnp.mean(values * values, axis=-1, keepdims=True) + EPSILON)
    return (values * factor, factor)


def contract(left, right, left_dim, right_dim):
    return lax.dot_general(
        left, right, (((left_dim,), (right_dim,)), ((), ())), preferred_element_type=F32
    )


def tie(values, done):
    done = tuple(done)
    if not done:
        return list(values)
    return list(lax.optimization_barrier((tuple(values), done))[0])


class Shares:
    def __init__(self, count):
        self.count = count
        self.index = lax.axis_index("dp")
        self.bits = [1 << i for i in range(count.bit_length() - 1)]
        even = [0]
        for bit in self.bits[1:]:
            even = even + [k ^ bit for k in even]
        self.order = even + [k ^ 1 for k in even] if count > 1 else even

    def swap(self, value, bit):
        return lax.ppermute(value, "dp", [(i, i ^ bit) for i in range(self.count)])

    def relative(self, blocks):
        for bit in self.bits:
            odd = (self.index & bit) != 0
            blocks = [jnp.where(odd, blocks[k ^ bit], blocks[k]) for k in range(self.count)]
        return blocks

    def to_order(self, values):
        blocks = self.relative(jnp.split(values, self.count, axis=1))
        return jnp.concatenate([blocks[k] for k in self.order], axis=1)

    def from_order(self, values):
        parts = jnp.split(values, self.count, axis=1)
        blocks = [parts[self.order.index(k)] for k in range(self.count)]
        return jnp.concatenate(self.relative(blocks), axis=1)

    def gather(self, block, done=()):
        (value,) = tie([block], done)
        for bit in self.bits[1:]:
            value = jnp.concatenate([value, self.swap(value, bit)], axis=0)
        return value, self.swap(value, 1)

    def scatter_sum(self, kept, given):
        total = kept() + self.swap(given, 1).astype(F32)
        for bit in reversed(self.bits[1:]):
            half = total.shape[0] // 2
            low = total.astype(BF16)
            total = total[:half] + self.swap(low[half:], bit).astype(F32)
        return total.astype(BF16)


class Ring:
    def __init__(self, size):
        self.size = size
        self.order = list(range(0, size, 2)) + list(range(size - 1, 0, -2))
        places = [self.order.index(i) for i in range(size)]
        self.place = jnp.array(places, jnp.int32)[lax.axis_index("ctx")]
        self.table = jnp.array(self.order, jnp.int32)
        self.done = ()

    def owner(self, ahead):
        return self.table[lax.rem(self.place + ahead + self.size, self.size)]

    def owners(self):
        return jnp.roll(jnp.concatenate([self.table, self.table]), -self.place)[: self.size]

    def shift(self, value, by):
        pairs = [
            (self.order[i], self.order[(i + by) % self.size]) for i in range(self.size)
        ]
        return lax.ppermute(value, "ctx", pairs)

    def both(self, right, left, done=()):
        right, left = tie((right, left), (*self.done, *done))
        right, left = self.shift(right, 1), self.shift(left, -1)
        self.done = (right, left)
        return right, left

    def gather(self, value, fill=()):
        size, half = self.size, self.size // 2
        fill = dict(enumerate(fill))
        pieces = [None] * size
        pieces[0] = value
        right = left = value
        for step in range(1, half):
            right, left = self.both(right, left, fill.get(step - 1, ()))
            pieces[size - step] = right
            pieces[step] = left
        rows = value.shape[0] // 2
        pieces[half] = jnp.concatenate(
            self.both(right[:rows], left[rows:], fill.get(half - 1, ())), axis=0
        )
        return pieces

    def scatter_sum(self, lower, upper, fill=()):
        size, half = self.size, self.size // 2
        fill = dict(enumerate(fill))
        rows = lower.shape[0] // size

        def part(ahead, source):
            return source[ahead * rows : (ahead + 1) * rows]

        def whole(ahead):
            return jnp.concatenate([part(ahead, lower), part(ahead, upper)], axis=1)

        right, left = self.both(
            part(half, lower).astype(BF16), part(half, upper).astype(BF16), fill.get(0, ())
        )
        for step in range(1, half):
            if step == 1:
                right = jnp.concatenate(
                    [part(half - 1, lower) + right.astype(F32), part(half - 1, upper)], axis=1
                )
                left = jnp.concatenate(
                    [part(half + 1, lower), part(half + 1, upper) + left.astype(F32)], axis=1
                )
            else:
                right = whole(half - step) + right.astype(F32)
                left = whole(half + step) + left.astype(F32)
            right, left = self.both(right.astype(BF16), left.astype(BF16), fill.get(step, ()))
        if half == 1:
            return jnp.concatenate(
                [part(0, lower) + right.astype(F32), part(0, upper) + left.astype(F32)], axis=1
            )
        return whole(0) + right.astype(F32) + left.astype(F32)

    def exchange(self, pieces, done=()):
        size = self.size
        out = [None] * size
        out[0] = pieces[0]
        sent = tie(pieces[1:], done)
        for by in range(1, size):
            out[size - by] = self.shift(sent[by - 1], by)
        return out

    def place_in_order(self, pieces):
        out = jnp.zeros((self.size,) + pieces[0].shape, pieces[0].dtype)
        for ahead in range(self.size):
            out = lax.dynamic_update_index_in_dim(out, pieces[ahead], self.owner(ahead), 0)
        return out

    def take_relative(self, stacked):
        return [
            lax.dynamic_index_in_dim(stacked, self.owner(ahead), 0, keepdims=False)
            for ahead in range(self.size)
        ]


def column_blocks(weight, size):
    width = weight.shape[1] // size
    return jnp.stack([weight[:, i * width : (i + 1) * width] for i in range(size)])


def join_columns(stacked):
    return jnp.concatenate([stacked[i] for i in range(stacked.shape[0])], axis=1)


def swap_halves(values, half):
    width = values.shape[-1]
    if width == 2 * half:
        return jnp.concatenate([values[:, half:], values[:, :half]], axis=1)
    lane = lax.broadcasted_iota(jnp.int32, values.shape, 1)
    ahead = pltpu.roll(values, width - half, 1)
    behind = pltpu.roll(values, half, 1)
    return jnp.where(lax.rem(lane, 2 * half) < half, ahead, behind)


def head_only(values, lane, head, head_size):
    inside = (lane >= head * head_size) & (lane < (head + 1) * head_size)
    return jnp.where(inside, values, jnp.zeros_like(values))


def flat(ref):
    value = ref[...]
    return value.reshape((value.shape[0] * value.shape[1], value.shape[2]))


def forward_kernel(
    head_size, lengths_ref, q_ref, k_ref, v_ref, cq_ref, sq_ref, ck_ref, sk_ref, qp_ref, kp_ref,
    out_ref, qr_ref, kr_ref, vr_ref, lse_ref,
):
    length = lengths_ref[pl.program_id(0)]
    half = head_size // 2
    queries = flat(q_ref)
    keys = flat(k_ref)
    queries = (queries * cq_ref[...] + swap_halves(queries, half) * sq_ref[...]).astype(BF16)
    keys = (keys * ck_ref[...] + swap_halves(keys, half) * sk_ref[...]).astype(BF16)
    values = flat(v_ref).astype(BF16)
    qr_ref[...] = queries.reshape(qr_ref.shape)
    kr_ref[...] = keys.reshape(kr_ref.shape)
    vr_ref[...] = values.reshape(vr_ref.shape)
    rows, width = queries.shape
    lane = lax.broadcasted_iota(jnp.int32, (rows, width), 1)
    query_pos = qp_ref[:, 0:1]
    key_pos = kp_ref[0:1, :]
    allowed = (key_pos <= query_pos) & (key_pos < length)
    total = jnp.zeros((rows, width), F32)
    scale = head_size ** (-0.5)
    for head in range(width // head_size):
        one = head_only(queries, lane, head, head_size)
        scores = contract(one, keys, 1, 1) * scale
        masked = jnp.where(allowed, scores, NEGATIVE)
        peak = jnp.max(masked, axis=-1, keepdims=True)
        weights = jnp.where(allowed, jnp.exp(masked - peak), 0.0)
        mass = jnp.sum(weights, axis=-1, keepdims=True)
        lse_ref[:, head : head + 1] = peak + jnp.log(mass)
        mixed = contract(weights.astype(BF16), values, 1, 0) / mass
        total = total + head_only(mixed, lane, head, head_size)
    out_ref[...] = total.astype(BF16).reshape(out_ref.shape)


def backward_kernel(
    head_size, lengths_ref, q_ref, k_ref, v_ref, g_ref, lse_ref, cq_ref, sq_ref, ck_ref, sk_ref, qp_ref,
    kp_ref, dq_ref, dk_ref, dv_ref, dk_sum, dv_sum,
):
    length = lengths_ref[pl.program_id(0)]
    half = head_size // 2
    queries, keys, values, grads = flat(q_ref), flat(k_ref), flat(v_ref), flat(g_ref)
    rows, width = queries.shape
    lane = lax.broadcasted_iota(jnp.int32, (rows, width), 1)
    allowed = (kp_ref[0:1, :] <= qp_ref[:, 0:1]) & (kp_ref[0:1, :] < length)
    scale = head_size ** (-0.5)

    @pl.when(pl.program_id(1) == 0)
    def start():
        dk_sum[...] = jnp.zeros_like(dk_sum)
        dv_sum[...] = jnp.zeros_like(dv_sum)

    dq = jnp.zeros((rows, width), F32)
    for head in range(width // head_size):
        one = head_only(queries, lane, head, head_size)
        grad = head_only(grads, lane, head, head_size)
        scores = contract(one, keys, 1, 1) * scale
        prob = jnp.where(
            allowed,
            jnp.exp(jnp.where(allowed, scores, NEGATIVE) - lse_ref[:, head : head + 1]),
            0.0,
        )
        grad_prob = contract(grad, values, 1, 1)
        delta = jnp.sum(prob * grad_prob, axis=-1, keepdims=True)
        grad_score = (prob * (grad_prob - delta) * scale).astype(BF16)
        dq = dq + head_only(contract(grad_score, keys, 1, 0), lane, head, head_size)
        dk_sum[...] += contract(grad_score, one, 0, 0)
        dv_sum[...] += contract(prob.astype(BF16), grad, 0, 0)
    dq = dq * cq_ref[...] - swap_halves(dq, half) * sq_ref[...]
    dq_ref[...] = dq.astype(BF16).reshape(dq_ref.shape)

    @pl.when(pl.program_id(1) == pl.num_programs(1) - 1)
    def finish():
        dk = dk_sum[...]
        dk = dk * ck_ref[...] - swap_halves(dk, half) * sk_ref[...]
        dk_ref[...] = dk.astype(BF16).reshape(dk_ref.shape)
        dv_ref[...] = dv_sum[...].astype(BF16).reshape(dv_ref.shape)


class Attention:
    def __init__(self, size, groups, slots, width, head_size, lengths, owners):
        self.size, self.groups, self.slots, self.width = size, groups, slots, width
        self.head_size = head_size
        self.lengths = lengths
        self.heads = width // head_size
        self.steps = max(1, min(size, QUERY_ROWS // slots))
        half = head_size // 2
        positions = (owners[:, None] * slots + jnp.arange(slots, dtype=jnp.int32)[None]).reshape(-1)
        freqs = THETA ** (-(jnp.arange(half, dtype=F32) * 2.0) / (2.0 * half))
        angles = positions.astype(F32)[:, None] * freqs[None, :]
        cosine, sine = jnp.cos(angles), jnp.sin(angles)
        self.cosine = jnp.tile(cosine, (1, 2 * self.heads))
        self.sine = jnp.tile(jnp.concatenate([-sine, sine], axis=1), (1, self.heads))
        self.query_pos = jnp.broadcast_to(positions[:, None], (positions.shape[0], 128))
        self.key_pos = jnp.broadcast_to(positions[None, :], (8, positions.shape[0]))
        total = size * slots
        rows = self.steps * slots
        self.grid = (groups, size // self.steps)
        self.q_spec = self.tokens(self.steps, width, 0, True)
        self.k_spec = self.tokens(size, width, 0, False)
        self.table_q = pl.BlockSpec((rows, width), lambda b, i, *_: (i, 0))
        self.table_k = pl.BlockSpec((total, width), lambda b, i, *_: (0, 0))
        self.pos_q = pl.BlockSpec((rows, 128), lambda b, i, *_: (i, 0))
        self.pos_k = pl.BlockSpec((8, total), lambda b, i, *_: (0, 0))
        self.lse = pl.BlockSpec((None, rows, self.heads), lambda b, i, *_: (b, i, 0))
        self.lse_shape = jax.ShapeDtypeStruct((groups, total, self.heads), F32)
        self.shape = jax.ShapeDtypeStruct((size, groups, slots, width), BF16)
        self.work = groups * self.heads * total * total

    def tokens(self, count, width, column, moving):
        return pl.BlockSpec(
            (count, None, self.slots, width),
            (lambda b, i, *_: (i, b, 0, column)) if moving else (lambda b, i, *_: (0, b, 0, column)),
        )

    def split(self, array):
        return array.reshape(self.size, self.groups, self.slots, -1)

    def cost(self, matmuls):
        return pl.CostEstimate(
            flops=2 * matmuls * self.work * self.head_size,
            transcendentals=self.work,
            bytes_accessed=8 * self.size * self.groups * self.slots * self.width * 2,
        )

    def forward(self, projected):
        width = self.width
        if width % 128 == 0:
            arrays = (self.split(projected),) * 3
            columns = (0, 1, 2)
        else:
            arrays = tuple(
                self.split(projected[:, i * width : (i + 1) * width]) for i in range(3)
            )
            columns = (0, 0, 0)
        return pl.pallas_call(
            functools.partial(forward_kernel, self.head_size),
            grid_spec=pltpu.PrefetchScalarGridSpec(
                num_scalar_prefetch=1,
                grid=self.grid,
                in_specs=[
                    self.tokens(self.steps, width, columns[0], True),
                    self.tokens(self.size, width, columns[1], False),
                    self.tokens(self.size, width, columns[2], False),
                    self.table_q, self.table_q, self.table_k, self.table_k, self.pos_q, self.pos_k,
                ],
                out_specs=[self.q_spec, self.q_spec, self.k_spec, self.k_spec, self.lse],
            ),
            out_shape=[self.shape] * 4 + [self.lse_shape],
            cost_estimate=self.cost(2),
            name="attention_forward",
        )(
            self.lengths, *arrays, self.cosine, self.sine, self.cosine, self.sine, self.query_pos, self.key_pos
        )

    def backward(self, queries, keys, values, grads, lse):
        total = self.size * self.slots
        return pl.pallas_call(
            functools.partial(backward_kernel, self.head_size),
            grid_spec=pltpu.PrefetchScalarGridSpec(
                num_scalar_prefetch=1,
                grid=self.grid,
                in_specs=[
                    self.q_spec, self.k_spec, self.k_spec, self.q_spec, self.lse,
                    self.table_q, self.table_q, self.table_k, self.table_k, self.pos_q, self.pos_k,
                ],
                out_specs=[self.q_spec, self.k_spec, self.k_spec],
                scratch_shapes=[pltpu.VMEM((total, self.width), F32)] * 2,
            ),
            out_shape=[self.shape] * 3,
            cost_estimate=self.cost(5),
            name="attention_backward",
        )(
            self.lengths, queries, keys, values, self.split(grads), lse,
            self.cosine, self.sine, self.cosine, self.sine, self.query_pos, self.key_pos,
        )


def body(
    inputs, cotangent, lengths, query_weight, key_weight, value_weight, mix_weight, gate_weight,
    up_weight, down_weight, attn_gain, ffn_gain,
):
    groups, slots, width = inputs.shape
    head_size = width // HEADS
    size = lax.axis_size("ctx")
    count = lax.axis_size("dp")
    rows = groups * slots
    ring = Ring(size)
    shares = Shares(count)
    owners = ring.owners()
    local = width // size
    hidden_local = gate_weight.shape[1] // size
    gain_one = attn_gain.astype(F32)[:, None]
    gain_two = ffn_gain.astype(F32)[:, None]

    def scaled(weight, gain):
        return (weight.astype(F32) * gain).astype(BF16)

    def send_columns(weights, done=()):
        blocks = jnp.concatenate([column_blocks(w, size) for w in weights], axis=2)
        return ring.exchange(ring.take_relative(blocks), done)

    def placed(pieces):
        got = ring.place_in_order(pieces)
        return got.reshape(-1, got.shape[2])

    def halves(pieces):
        half = width // 2
        return (
            jnp.concatenate([p[:, :half] for p in pieces], axis=0),
            jnp.concatenate([p[:, half:] for p in pieces], axis=0),
        )

    def apply(values, weights):
        return contract(values[0], weights[0], 1, 0) + contract(values[1], weights[1], 1, 0)

    block_in = shares.to_order(inputs.reshape(rows, width)).astype(F32)
    positions = lax.axis_index("ctx") * slots + jnp.arange(slots, dtype=jnp.int32)
    valid = (positions[None, :] < lengths[:, None]).astype(F32).reshape(rows, 1)
    normed_one, factor_one = normalize(block_in)
    grad_out = shares.to_order(cotangent.reshape(rows, width)).astype(F32) * valid

    attn_pieces = send_columns([scaled(w, gain_one) for w in (query_weight, key_weight, value_weight)])
    one_pieces = ring.gather(normed_one.astype(BF16))
    one_all = halves(one_pieces)
    attn_weights = shares.gather(placed(attn_pieces))
    to_shares = [(i * size + j, j * count + i) for i in range(count) for j in range(size)]
    from_shares = [(there, here) for here, there in to_shares]
    (mix_sent,) = tie([mix_weight], ring.done)
    mix_parts = shares.gather(lax.ppermute(mix_sent, ("dp", "ctx"), from_shares))
    ffn_pieces = send_columns(
        [scaled(gate_weight, gain_two), scaled(up_weight, gain_two), down_weight], ring.done
    )
    mix_blocks = jnp.split(jnp.concatenate(mix_parts, axis=0), count, axis=0)
    mix_rows = shares.to_order(
        jnp.concatenate(
            shares.relative([mix_blocks[shares.order.index(k)] for k in range(count)]), axis=0
        )
    )
    projected = apply(one_all, attn_weights)
    attention = Attention(size, groups, slots, local, head_size, lengths, owners)
    mixed, query_rot, key_rot, value_low, lse = attention.forward(projected)
    mixed = mixed.reshape(size * rows, local)
    attn_out = contract(mixed, mix_rows, 1, 0)
    residual = block_in + ring.scatter_sum(attn_out[:, : width // 2], attn_out[:, width // 2 :])

    ffn_weights = shares.gather(placed([p[:, : 2 * hidden_local] for p in ffn_pieces]))
    down_weights = shares.gather(
        placed([p[:, 2 * hidden_local :] for p in ffn_pieces]), [ffn_weights[1]]
    )
    normed_two, factor_two = normalize(residual)
    two_all = halves(ring.gather(normed_two.astype(BF16)))
    grad_all = halves(ring.gather(grad_out.astype(BF16)))
    gate_up = apply(two_all, ffn_weights)
    gate, up = gate_up[:, :hidden_local], gate_up[:, hidden_local:]
    sigma = jax.nn.sigmoid(gate)
    silu_gate = gate * sigma
    hidden = (silu_gate * up).astype(BF16)
    branch = ring.scatter_sum(*(contract(hidden, w, 1, 1) for w in down_weights))
    activations = valid * (residual + branch)

    grad_hidden = apply(grad_all, down_weights)
    grad_both = jnp.concatenate(
        [
            (grad_hidden * up * sigma * (1.0 + gate * (1.0 - sigma))).astype(BF16),
            (grad_hidden * silu_gate).astype(BF16),
        ],
        axis=1,
    )

    def summed(values, gradient):
        given = contract(values[1], gradient, 0, 0).astype(BF16)
        return given, lambda: shares.scatter_sum(
            lambda: contract(values[0], gradient, 0, 0), given
        )

    down_given, down_total = summed(grad_all, hidden)
    both_given, both_total = summed(two_all, grad_both)
    down_sum = down_total()
    both_sum = both_total()
    scaled_two = ring.scatter_sum(
        *(contract(grad_both, w, 1, 1) for w in ffn_weights),
        fill=((), (down_given,), (both_given,)),
    )
    dres = grad_out + factor_two * (
        scaled_two - normed_two * jnp.mean(normed_two * scaled_two, axis=-1, keepdims=True)
    )
    dres_low = dres.astype(BF16)

    def send_rows(total, done=()):
        stacked = total.reshape(size, total.shape[0] // size, total.shape[1])
        return ring.exchange(ring.take_relative(stacked), done)

    dres_pieces = ring.gather(dres_low, fill=((), (), (down_sum,)))
    dres_all = jnp.concatenate(dres_pieces, axis=0)
    down_pieces = send_rows(down_sum, ring.done)
    both_pieces = send_rows(both_sum, ring.done)
    grad_heads = contract(dres_all, mix_rows, 1, 1).astype(BF16)
    dq, dk, dv = attention.backward(query_rot, key_rot, value_low, grad_heads, lse)
    projected_grad = jnp.concatenate(
        [d.reshape(size * rows, local) for d in (dq, dk, dv)], axis=1
    )
    attn_given, attn_total = summed(one_all, projected_grad)
    attn_sum = attn_total()
    attn_pieces = send_rows(attn_sum)
    mix_terms = shares.from_order(contract(mixed, dres_all, 0, 0))
    mix_blocks = shares.relative(jnp.split(mix_terms, count, axis=0))
    mix_blocks = [mix_blocks[k] for k in shares.order]
    mix_given = jnp.concatenate(mix_blocks[count // 2 :], axis=0).astype(BF16)
    mix_sum = shares.scatter_sum(
        lambda: jnp.concatenate(mix_blocks[: count // 2], axis=0), mix_given
    )
    scaled_one = ring.scatter_sum(
        *(contract(projected_grad, w, 1, 1) for w in attn_weights),
        fill=((attn_given,),),
    )
    input_grad = dres + factor_one * (
        scaled_one - normed_one * jnp.mean(normed_one * scaled_one, axis=-1, keepdims=True)
    )
    mix_grad = lax.ppermute(mix_sum, ("dp", "ctx"), to_shares).astype(F32)

    def joined(pieces, columns):
        return join_columns(ring.place_in_order([p[:, columns] for p in pieces])).astype(F32)

    down_grad = joined(down_pieces, slice(None))
    gate_raw = joined(both_pieces, slice(0, hidden_local))
    up_raw = joined(both_pieces, slice(hidden_local, 2 * hidden_local))
    query_raw, key_raw, value_raw = (
        joined(attn_pieces, slice(i * local, (i + 1) * local)) for i in range(3)
    )

    def row_sum(*pairs):
        return sum(jnp.sum(w.astype(F32) * g, axis=1) for w, g in pairs)

    attn_gain_grad = row_sum(
        (query_weight, query_raw), (key_weight, key_raw), (value_weight, value_raw)
    )
    ffn_gain_grad = row_sum((gate_weight, gate_raw), (up_weight, up_raw))
    return (
        shares.from_order(activations.astype(BF16)).reshape(groups, slots, width),
        shares.from_order(input_grad.astype(BF16)).reshape(groups, slots, width),
        query_raw * gain_one,
        key_raw * gain_one,
        value_raw * gain_one,
        mix_grad,
        gate_raw * gain_two,
        up_raw * gain_two,
        down_grad,
        attn_gain_grad,
        ffn_gain_grad,
    )


def solution(mesh):
    rows = P(("dp", "ctx"), None)
    tokens = P("dp", "ctx", None)
    gains = P(("dp", "ctx"))
    return jax.shard_map(
        body,
        mesh=mesh,
        in_specs=(tokens, tokens, P("dp")) + (rows,) * 7 + (gains, gains),
        out_specs=(tokens, tokens) + (rows,) * 7 + (gains, gains),
        check_vma=False,
    )
```

```python
import functools

import jax
import jax.numpy as jnp
from jax import lax
from jax.experimental import pallas as pl
from jax.experimental.pallas import tpu as pltpu
from jax.sharding import PartitionSpec as P

HEADS = 32
EPSILON = 1e-05
THETA = 130000.0
NEGATIVE = -1e30
QUERY_ROWS = 512
BF16 = jnp.bfloat16
F32 = jnp.float32


def normalize(values):
    factor = lax.rsqrt(jnp.mean(values * values, axis=-1, keepdims=True) + EPSILON)
    return (values * factor, factor)


def contract(left, right, left_dim, right_dim):
    return lax.dot_general(
        left, right, (((left_dim,), (right_dim,)), ((), ())), preferred_element_type=F32
    )


def tie(values, done):
    done = tuple(done)
    if not done:
        return list(values)
    return list(lax.optimization_barrier((tuple(values), done))[0])


class Shares:
    def __init__(self, count):
        self.count = count
        self.index = lax.axis_index("dp")
        self.bits = [1 << i for i in range(count.bit_length() - 1)]
        even = [0]
        for bit in self.bits[1:]:
            even = even + [k ^ bit for k in even]
        self.order = even + [k ^ 1 for k in even] if count > 1 else even

    def swap(self, value, bit):
        return lax.ppermute(value, "dp", [(i, i ^ bit) for i in range(self.count)])

    def relative(self, blocks):
        for bit in self.bits:
            odd = (self.index & bit) != 0
            blocks = [jnp.where(odd, blocks[k ^ bit], blocks[k]) for k in range(self.count)]
        return blocks

    def to_order(self, values):
        blocks = self.relative(jnp.split(values, self.count, axis=1))
        return jnp.concatenate([blocks[k] for k in self.order], axis=1)

    def from_order(self, values):
        parts = jnp.split(values, self.count, axis=1)
        blocks = [parts[self.order.index(k)] for k in range(self.count)]
        return jnp.concatenate(self.relative(blocks), axis=1)

    def gather(self, block, done=(), later=()):
        (value,) = tie([block], done)
        for bit in self.bits[1:]:
            value = jnp.concatenate([value, *tie([self.swap(value, bit)], later)], axis=0)
        return value, self.swap(value, 1)

    def scatter_sum(self, kept, given):
        total = kept() + self.swap(given, 1).astype(F32)
        for bit in reversed(self.bits[1:]):
            half = total.shape[0] // 2
            low = total.astype(BF16)
            total = total[:half] + self.swap(low[half:], bit).astype(F32)
        return total.astype(BF16)


class Ring:
    def __init__(self, size):
        self.size = size
        self.order = list(range(0, size, 2)) + list(range(size - 1, 0, -2))
        index = lax.axis_index("ctx")
        self.place = jnp.where(index % 2 == 0, index // 2, size - (index + 1) // 2)
        self.done = ()
        self.steps = []

    def owner(self, ahead):
        place = lax.rem(self.place + ahead, self.size)
        return jnp.where(place < self.size // 2, 2 * place, 2 * (self.size - place) - 1)

    def owners(self):
        return self.owner(jnp.arange(self.size, dtype=jnp.int32))

    def shift(self, value, by):
        pairs = [
            (self.order[i], self.order[(i + by) % self.size]) for i in range(self.size)
        ]
        return lax.ppermute(value, "ctx", pairs)

    def both(self, right, left, done=()):
        right, left = tie((right, left), (*self.done, *done))
        right, left = self.shift(right, 1), self.shift(left, -1)
        self.done = (right, left)
        self.steps.append(self.done)
        return right, left

    def gather(self, value, fill=()):
        size, half = self.size, self.size // 2
        fill = dict(enumerate(fill))
        pieces = [None] * size
        pieces[0] = value
        right = left = value
        for step in range(1, half):
            right, left = self.both(right, left, fill.get(step - 1, ()))
            pieces[size - step] = right
            pieces[step] = left
        rows = value.shape[0] // 2
        pieces[half] = jnp.concatenate(
            self.both(right[:rows], left[rows:], fill.get(half - 1, ())), axis=0
        )
        return pieces

    def scatter_sum(self, lower, upper, fill=()):
        size, half = self.size, self.size // 2
        fill = dict(enumerate(fill))
        rows = lower.shape[0] // size

        def part(ahead, source):
            return source[ahead * rows : (ahead + 1) * rows]

        def whole(ahead):
            return jnp.concatenate([part(ahead, lower), part(ahead, upper)], axis=1)

        right, left = self.both(
            part(half, lower).astype(BF16), part(half, upper).astype(BF16), fill.get(0, ())
        )
        for step in range(1, half):
            if step == 1:
                right = jnp.concatenate(
                    [part(half - 1, lower) + right.astype(F32), part(half - 1, upper)], axis=1
                )
                left = jnp.concatenate(
                    [part(half + 1, lower), part(half + 1, upper) + left.astype(F32)], axis=1
                )
            else:
                right = whole(half - step) + right.astype(F32)
                left = whole(half + step) + left.astype(F32)
            right, left = self.both(right.astype(BF16), left.astype(BF16), fill.get(step, ()))
        if half == 1:
            return jnp.concatenate(
                [part(0, lower) + right.astype(F32), part(0, upper) + left.astype(F32)], axis=1
            )
        return whole(0) + right.astype(F32) + left.astype(F32)

    def exchange(self, pieces, done=()):
        size = self.size
        out = [None] * size
        out[0] = pieces[0]
        sent = tie(pieces[1:], done)
        for by in range(1, size):
            out[size - by] = self.shift(sent[by - 1], by)
        return out

    def place_in_order(self, pieces):
        out = jnp.zeros((self.size,) + pieces[0].shape, pieces[0].dtype)
        for ahead in range(self.size):
            out = lax.dynamic_update_index_in_dim(out, pieces[ahead], self.owner(ahead), 0)
        return out

    def take_relative(self, stacked):
        return [
            lax.dynamic_index_in_dim(stacked, self.owner(ahead), 0, keepdims=False)
            for ahead in range(self.size)
        ]


def column_blocks(weight, size):
    width = weight.shape[1] // size
    return jnp.stack([weight[:, i * width : (i + 1) * width] for i in range(size)])


def join_columns(stacked):
    return jnp.concatenate([stacked[i] for i in range(stacked.shape[0])], axis=1)


def swap_halves(values, half):
    width = values.shape[-1]
    if width == 2 * half:
        return jnp.concatenate([values[:, half:], values[:, :half]], axis=1)
    lane = lax.broadcasted_iota(jnp.int32, values.shape, 1)
    ahead = pltpu.roll(values, width - half, 1)
    behind = pltpu.roll(values, half, 1)
    return jnp.where(lax.rem(lane, 2 * half) < half, ahead, behind)


def head_only(values, lane, head, head_size):
    inside = (lane >= head * head_size) & (lane < (head + 1) * head_size)
    return jnp.where(inside, values, jnp.zeros_like(values))


def flat(ref):
    value = ref[...]
    return value.reshape((value.shape[0] * value.shape[1], value.shape[2]))


def forward_kernel(
    head_size, lengths_ref, q_ref, k_ref, v_ref, cq_ref, sq_ref, ck_ref, sk_ref, qp_ref, kp_ref,
    out_ref, qr_ref, kr_ref, vr_ref, lse_ref,
):
    length = lengths_ref[pl.program_id(0)]
    half = head_size // 2
    queries = flat(q_ref)
    keys = flat(k_ref)
    queries = (queries * cq_ref[...] + swap_halves(queries, half) * sq_ref[...]).astype(BF16)
    keys = (keys * ck_ref[...] + swap_halves(keys, half) * sk_ref[...]).astype(BF16)
    values = flat(v_ref).astype(BF16)
    qr_ref[...] = queries.reshape(qr_ref.shape)
    kr_ref[...] = keys.reshape(kr_ref.shape)
    vr_ref[...] = values.reshape(vr_ref.shape)
    rows, width = queries.shape
    lane = lax.broadcasted_iota(jnp.int32, (rows, width), 1)
    query_pos = qp_ref[:, 0:1]
    key_pos = kp_ref[0:1, :]
    allowed = (key_pos <= query_pos) & (key_pos < length)
    total = jnp.zeros((rows, width), F32)
    scale = head_size ** (-0.5)
    for head in range(width // head_size):
        one = head_only(queries, lane, head, head_size)
        scores = contract(one, keys, 1, 1) * scale
        masked = jnp.where(allowed, scores, NEGATIVE)
        peak = jnp.max(masked, axis=-1, keepdims=True)
        weights = jnp.where(allowed, jnp.exp(masked - peak), 0.0)
        mass = jnp.sum(weights, axis=-1, keepdims=True)
        lse_ref[:, head : head + 1] = peak + jnp.log(mass)
        mixed = contract(weights.astype(BF16), values, 1, 0) / mass
        total = total + head_only(mixed, lane, head, head_size)
    out_ref[...] = total.astype(BF16).reshape(out_ref.shape)


def backward_kernel(
    head_size, lengths_ref, q_ref, k_ref, v_ref, g_ref, lse_ref, cq_ref, sq_ref, ck_ref, sk_ref, qp_ref,
    kp_ref, dq_ref, dk_ref, dv_ref, dk_sum, dv_sum,
):
    length = lengths_ref[pl.program_id(0)]
    half = head_size // 2
    queries, keys, values, grads = flat(q_ref), flat(k_ref), flat(v_ref), flat(g_ref)
    rows, width = queries.shape
    lane = lax.broadcasted_iota(jnp.int32, (rows, width), 1)
    allowed = (kp_ref[0:1, :] <= qp_ref[:, 0:1]) & (kp_ref[0:1, :] < length)
    scale = head_size ** (-0.5)

    @pl.when(pl.program_id(1) == 0)
    def start():
        dk_sum[...] = jnp.zeros_like(dk_sum)
        dv_sum[...] = jnp.zeros_like(dv_sum)

    dq = jnp.zeros((rows, width), F32)
    for head in range(width // head_size):
        one = head_only(queries, lane, head, head_size)
        grad = head_only(grads, lane, head, head_size)
        scores = contract(one, keys, 1, 1) * scale
        prob = jnp.where(
            allowed,
            jnp.exp(jnp.where(allowed, scores, NEGATIVE) - lse_ref[:, head : head + 1]),
            0.0,
        )
        grad_prob = contract(grad, values, 1, 1)
        delta = jnp.sum(prob * grad_prob, axis=-1, keepdims=True)
        grad_score = (prob * (grad_prob - delta) * scale).astype(BF16)
        dq = dq + head_only(contract(grad_score, keys, 1, 0), lane, head, head_size)
        dk_sum[...] += contract(grad_score, one, 0, 0)
        dv_sum[...] += contract(prob.astype(BF16), grad, 0, 0)
    dq = dq * cq_ref[...] - swap_halves(dq, half) * sq_ref[...]
    dq_ref[...] = dq.astype(BF16).reshape(dq_ref.shape)

    @pl.when(pl.program_id(1) == pl.num_programs(1) - 1)
    def finish():
        dk = dk_sum[...]
        dk = dk * ck_ref[...] - swap_halves(dk, half) * sk_ref[...]
        dk_ref[...] = dk.astype(BF16).reshape(dk_ref.shape)
        dv_ref[...] = dv_sum[...].astype(BF16).reshape(dv_ref.shape)


class Attention:
    def __init__(self, size, groups, slots, width, head_size, lengths, owners):
        self.size, self.groups, self.slots, self.width = size, groups, slots, width
        self.head_size = head_size
        self.lengths = lengths
        self.heads = width // head_size
        self.steps = max(1, min(size, QUERY_ROWS // slots))
        half = head_size // 2
        positions = (owners[:, None] * slots + jnp.arange(slots, dtype=jnp.int32)[None]).reshape(-1)
        freqs = THETA ** (-(jnp.arange(half, dtype=F32) * 2.0) / (2.0 * half))
        angles = positions.astype(F32)[:, None] * freqs[None, :]
        cosine, sine = jnp.cos(angles), jnp.sin(angles)
        self.cosine = jnp.tile(cosine, (1, 2 * self.heads))
        self.sine = jnp.tile(jnp.concatenate([-sine, sine], axis=1), (1, self.heads))
        self.query_pos = jnp.broadcast_to(positions[:, None], (positions.shape[0], 128))
        self.key_pos = jnp.broadcast_to(positions[None, :], (8, positions.shape[0]))
        total = size * slots
        rows = self.steps * slots
        self.grid = (groups, size // self.steps)
        self.q_spec = self.tokens(self.steps, width, 0, True)
        self.k_spec = self.tokens(size, width, 0, False)
        self.table_q = pl.BlockSpec((rows, width), lambda b, i, *_: (i, 0))
        self.table_k = pl.BlockSpec((total, width), lambda b, i, *_: (0, 0))
        self.pos_q = pl.BlockSpec((rows, 128), lambda b, i, *_: (i, 0))
        self.pos_k = pl.BlockSpec((8, total), lambda b, i, *_: (0, 0))
        self.lse = pl.BlockSpec((None, rows, self.heads), lambda b, i, *_: (b, i, 0))
        self.lse_shape = jax.ShapeDtypeStruct((groups, total, self.heads), F32)
        self.shape = jax.ShapeDtypeStruct((size, groups, slots, width), BF16)
        self.work = groups * self.heads * total * total

    def tokens(self, count, width, column, moving):
        return pl.BlockSpec(
            (count, None, self.slots, width),
            (lambda b, i, *_: (i, b, 0, column)) if moving else (lambda b, i, *_: (0, b, 0, column)),
        )

    def split(self, array):
        return array.reshape(self.size, self.groups, self.slots, -1)

    def cost(self, matmuls):
        return pl.CostEstimate(
            flops=2 * matmuls * self.work * self.head_size,
            transcendentals=self.work,
            bytes_accessed=8 * self.size * self.groups * self.slots * self.width * 2,
        )

    def forward(self, projected):
        width = self.width
        if width % 128 == 0:
            arrays = (self.split(projected),) * 3
            columns = (0, 1, 2)
        else:
            arrays = tuple(
                self.split(projected[:, i * width : (i + 1) * width]) for i in range(3)
            )
            columns = (0, 0, 0)
        return pl.pallas_call(
            functools.partial(forward_kernel, self.head_size),
            grid_spec=pltpu.PrefetchScalarGridSpec(
                num_scalar_prefetch=1,
                grid=self.grid,
                in_specs=[
                    self.tokens(self.steps, width, columns[0], True),
                    self.tokens(self.size, width, columns[1], False),
                    self.tokens(self.size, width, columns[2], False),
                    self.table_q, self.table_q, self.table_k, self.table_k, self.pos_q, self.pos_k,
                ],
                out_specs=[self.q_spec, self.q_spec, self.k_spec, self.k_spec, self.lse],
            ),
            out_shape=[self.shape] * 4 + [self.lse_shape],
            cost_estimate=self.cost(2),
            name="attention_forward",
        )(
            self.lengths, *arrays, self.cosine, self.sine, self.cosine, self.sine, self.query_pos, self.key_pos
        )

    def backward(self, queries, keys, values, grads, lse):
        total = self.size * self.slots
        return pl.pallas_call(
            functools.partial(backward_kernel, self.head_size),
            grid_spec=pltpu.PrefetchScalarGridSpec(
                num_scalar_prefetch=1,
                grid=self.grid,
                in_specs=[
                    self.q_spec, self.k_spec, self.k_spec, self.q_spec, self.lse,
                    self.table_q, self.table_q, self.table_k, self.table_k, self.pos_q, self.pos_k,
                ],
                out_specs=[self.q_spec, self.k_spec, self.k_spec],
                scratch_shapes=[pltpu.VMEM((total, self.width), F32)] * 2,
            ),
            out_shape=[self.shape] * 3,
            cost_estimate=self.cost(5),
            name="attention_backward",
        )(
            self.lengths, queries, keys, values, self.split(grads), lse,
            self.cosine, self.sine, self.cosine, self.sine, self.query_pos, self.key_pos,
        )


def body(
    inputs, cotangent, lengths, query_weight, key_weight, value_weight, mix_weight, gate_weight,
    up_weight, down_weight, attn_gain, ffn_gain,
):
    groups, slots, width = inputs.shape
    head_size = width // HEADS
    size = lax.axis_size("ctx")
    count = lax.axis_size("dp")
    rows = groups * slots
    ring = Ring(size)
    shares = Shares(count)
    owners = ring.owners()
    local = width // size
    hidden_local = gate_weight.shape[1] // size
    gain_one = attn_gain.astype(F32)[:, None]
    gain_two = ffn_gain.astype(F32)[:, None]

    def scaled(weight, gain):
        return (weight.astype(F32) * gain).astype(BF16)

    def send_columns(weights, done=()):
        blocks = jnp.concatenate([column_blocks(w, size) for w in weights], axis=2)
        return ring.exchange(ring.take_relative(blocks), done)

    def placed(pieces):
        got = ring.place_in_order(pieces)
        return got.reshape(-1, got.shape[2])

    def halves(pieces):
        half = width // 2
        return (
            jnp.concatenate([p[:, :half] for p in pieces], axis=0),
            jnp.concatenate([p[:, half:] for p in pieces], axis=0),
        )

    def apply(values, weights):
        return contract(values[0], weights[0], 1, 0) + contract(values[1], weights[1], 1, 0)

    block_in = shares.to_order(inputs.reshape(rows, width)).astype(F32)
    positions = lax.axis_index("ctx") * slots + jnp.arange(slots, dtype=jnp.int32)
    valid = (positions[None, :] < lengths[:, None]).astype(F32).reshape(rows, 1)
    normed_one, factor_one = normalize(block_in)
    grad_out = shares.to_order(cotangent.reshape(rows, width)).astype(F32) * valid

    to_shares = [(i * size + j, j * count + i) for i in range(count) for j in range(size)]
    from_shares = [(there, here) for here, there in to_shares]
    attn_pieces = send_columns([scaled(w, gain_one) for w in (query_weight, key_weight, value_weight)])
    mix_share = lax.ppermute(mix_weight, ("dp", "ctx"), from_shares)
    one_pieces = ring.gather(normed_one.astype(BF16))
    one_all = halves(one_pieces)
    attn_weights = shares.gather(placed(attn_pieces))
    ffn_pieces = send_columns(
        [scaled(gate_weight, gain_two), scaled(up_weight, gain_two)], ring.steps[-2]
    )
    mix_parts = shares.gather(mix_share, attn_weights[1:])
    mix_blocks = jnp.split(jnp.concatenate(mix_parts, axis=0), count, axis=0)
    mix_rows = shares.to_order(
        jnp.concatenate(
            shares.relative([mix_blocks[shares.order.index(k)] for k in range(count)]), axis=0
        )
    )
    projected = apply(one_all, attn_weights)
    attention = Attention(size, groups, slots, local, head_size, lengths, owners)
    mixed, query_rot, key_rot, value_low, lse = attention.forward(projected)
    mixed = mixed.reshape(size * rows, local)
    attn_out = contract(mixed, mix_rows, 1, 0)
    residual = block_in + ring.scatter_sum(attn_out[:, : width // 2], attn_out[:, width // 2 :])

    down_pieces = send_columns([down_weight], ring.steps[-2])
    normed_two, factor_two = normalize(residual)
    two_all = halves(ring.gather(normed_two.astype(BF16)))
    ffn_weights = shares.gather(placed(ffn_pieces), later=ring.steps[-2])
    low_part = contract(two_all[0], ffn_weights[0], 1, 0)
    gate_up = low_part + contract(two_all[1], ffn_weights[1], 1, 0)
    gate, up = gate_up[:, :hidden_local], gate_up[:, hidden_local:]
    sigma = jax.nn.sigmoid(gate)
    silu_gate = gate * sigma
    hidden = (silu_gate * up).astype(BF16)
    grad_all = halves(
        ring.gather(grad_out.astype(BF16), fill=((), (low_part,), (gate_up,), (hidden,)))
    )
    down_weights = shares.gather(
        placed(tie(down_pieces, ring.steps[-4])), ffn_weights[1:], later=(hidden,)
    )
    branch = ring.scatter_sum(*(contract(hidden, w, 1, 1) for w in down_weights))
    activations = valid * (residual + branch)

    grad_hidden = apply(grad_all, down_weights)
    grad_both = jnp.concatenate(
        [
            (grad_hidden * up * sigma * (1.0 + gate * (1.0 - sigma))).astype(BF16),
            (grad_hidden * silu_gate).astype(BF16),
        ],
        axis=1,
    )

    def summed(values, gradient):
        given = contract(values[1], gradient, 0, 0).astype(BF16)
        return given, lambda: shares.scatter_sum(
            lambda: contract(values[0], gradient, 0, 0), given
        )

    down_given, down_total = summed(grad_all, hidden)
    both_given, both_total = summed(two_all, grad_both)
    down_sum = down_total()
    both_sum = both_total()
    scaled_two = ring.scatter_sum(
        *(contract(grad_both, w, 1, 1) for w in ffn_weights),
        fill=((), (down_given,), (both_given,)),
    )
    dres = grad_out + factor_two * (
        scaled_two - normed_two * jnp.mean(normed_two * scaled_two, axis=-1, keepdims=True)
    )
    dres_low = dres.astype(BF16)

    def send_rows(total, done=()):
        stacked = total.reshape(size, total.shape[0] // size, total.shape[1])
        return ring.exchange(ring.take_relative(stacked), done)

    dres_pieces = ring.gather(dres_low, fill=((), (), (down_sum,)))
    dres_all = jnp.concatenate(dres_pieces, axis=0)
    down_pieces = send_rows(down_sum, ring.done)
    both_pieces = send_rows(both_sum, ring.done)
    grad_heads = contract(dres_all, mix_rows, 1, 1).astype(BF16)
    dq, dk, dv = attention.backward(query_rot, key_rot, value_low, grad_heads, lse)
    projected_grad = jnp.concatenate(
        [d.reshape(size * rows, local) for d in (dq, dk, dv)], axis=1
    )
    attn_given, attn_total = summed(one_all, projected_grad)
    attn_sum = attn_total()
    mix_terms = shares.from_order(contract(mixed, dres_all, 0, 0))
    mix_blocks = shares.relative(jnp.split(mix_terms, count, axis=0))
    mix_blocks = [mix_blocks[k] for k in shares.order]
    mix_given = jnp.concatenate(mix_blocks[count // 2 :], axis=0).astype(BF16)
    mix_sum = shares.scatter_sum(
        lambda: jnp.concatenate(mix_blocks[: count // 2], axis=0), mix_given
    )
    scaled_one = ring.scatter_sum(
        *(contract(projected_grad, w, 1, 1) for w in attn_weights),
        fill=((attn_given,),),
    )
    input_grad = dres + factor_one * (
        scaled_one - normed_one * jnp.mean(normed_one * scaled_one, axis=-1, keepdims=True)
    )
    attn_pieces = send_rows(attn_sum, ring.steps[-2])
    mix_grad = lax.ppermute(mix_sum, ("dp", "ctx"), to_shares).astype(F32)

    def joined(pieces, columns):
        return join_columns(ring.place_in_order([p[:, columns] for p in pieces])).astype(F32)

    down_pieces, both_pieces = (tie(p, ring.done) for p in (down_pieces, both_pieces))
    down_grad = joined(down_pieces, slice(None))
    gate_raw = joined(both_pieces, slice(0, hidden_local))
    up_raw = joined(both_pieces, slice(hidden_local, 2 * hidden_local))
    query_raw, key_raw, value_raw = (
        joined(attn_pieces, slice(i * local, (i + 1) * local)) for i in range(3)
    )

    def row_sum(*pairs):
        return sum(jnp.sum(w.astype(F32) * g, axis=1) for w, g in pairs)

    attn_gain_grad = row_sum(
        (query_weight, query_raw), (key_weight, key_raw), (value_weight, value_raw)
    )
    ffn_gain_grad = row_sum((gate_weight, gate_raw), (up_weight, up_raw))
    return (
        shares.from_order(activations.astype(BF16)).reshape(groups, slots, width),
        shares.from_order(input_grad.astype(BF16)).reshape(groups, slots, width),
        query_raw * gain_one,
        key_raw * gain_one,
        value_raw * gain_one,
        mix_grad,
        gate_raw * gain_two,
        up_raw * gain_two,
        down_grad,
        attn_gain_grad,
        ffn_gain_grad,
    )


def solution(mesh):
    rows = P(("dp", "ctx"), None)
    tokens = P("dp", "ctx", None)
    gains = P(("dp", "ctx"))
    return jax.shard_map(
        body,
        mesh=mesh,
        in_specs=(tokens, tokens, P("dp")) + (rows,) * 7 + (gains, gains),
        out_specs=(tokens, tokens) + (rows,) * 7 + (gains, gains),
        check_vma=False,
    )
```

```python
import functools

import jax
import jax.numpy as jnp
from jax import lax
from jax.experimental import pallas as pl
from jax.experimental.pallas import tpu as pltpu
from jax.sharding import PartitionSpec as P

HEADS = 32
EPSILON = 1e-05
THETA = 130000.0
NEGATIVE = -1e30
QUERY_ROWS = 512
BF16 = jnp.bfloat16
F32 = jnp.float32


def normalize(values):
    factor = lax.rsqrt(jnp.mean(values * values, axis=-1, keepdims=True) + EPSILON)
    return (values * factor, factor)


def contract(left, right, left_dim, right_dim):
    return lax.dot_general(
        left, right, (((left_dim,), (right_dim,)), ((), ())), preferred_element_type=F32
    )


def tie(values, done):
    done = tuple(done)
    if not done:
        return list(values)
    return list(lax.optimization_barrier((tuple(values), done))[0])


class Shares:
    def __init__(self, count):
        self.count = count
        self.index = lax.axis_index("dp")
        self.bits = [1 << i for i in range(count.bit_length() - 1)]
        even = [0]
        for bit in self.bits[1:]:
            even = even + [k ^ bit for k in even]
        self.order = even + [k ^ 1 for k in even] if count > 1 else even

    def swap(self, value, bit):
        return lax.ppermute(value, "dp", [(i, i ^ bit) for i in range(self.count)])

    def relative(self, blocks):
        for bit in self.bits:
            odd = (self.index & bit) != 0
            blocks = [jnp.where(odd, blocks[k ^ bit], blocks[k]) for k in range(self.count)]
        return blocks

    def to_order(self, values):
        blocks = self.relative(jnp.split(values, self.count, axis=1))
        return jnp.concatenate([blocks[k] for k in self.order], axis=1)

    def from_order(self, values):
        parts = jnp.split(values, self.count, axis=1)
        blocks = [parts[self.order.index(k)] for k in range(self.count)]
        return jnp.concatenate(self.relative(blocks), axis=1)

    def gather_far(self, block, done=()):
        (value,) = tie([block], done)
        for bit in self.bits[1:]:
            value = jnp.concatenate([value, self.swap(value, bit)], axis=0)
        return value

    def gather(self, block, done=()):
        value = self.gather_far(block, done)
        return value, self.swap(value, 1)

    def scatter_core(self, kept, given):
        return kept + self.swap(given, 1).astype(F32)

    def scatter_rest(self, total):
        for bit in reversed(self.bits[1:]):
            half = total.shape[0] // 2
            low = total[half:].astype(BF16)
            total = total[:half] + self.swap(low, bit).astype(F32)
        return total.astype(BF16)


class Ring:
    def __init__(self, size):
        self.size = size
        self.order = list(range(0, size, 2)) + list(range(size - 1, 0, -2))
        index = lax.axis_index("ctx")
        self.place = jnp.where(index % 2 == 0, index // 2, size - (index + 1) // 2)
        self.done = ()
        self.steps = []

    def owner(self, ahead):
        place = lax.rem(self.place + ahead, self.size)
        return jnp.where(place < self.size // 2, 2 * place, 2 * (self.size - place) - 1)

    def owners(self):
        return self.owner(jnp.arange(self.size, dtype=jnp.int32))

    def shift(self, value, by):
        pairs = [
            (self.order[i], self.order[(i + by) % self.size]) for i in range(self.size)
        ]
        return lax.ppermute(value, "ctx", pairs)

    def both(self, right, left, done=()):
        right, left = tie((right, left), (*self.done, *done))
        right, left = self.shift(right, 1), self.shift(left, -1)
        self.done = (right, left)
        self.steps.append(self.done)
        return right, left

    def gather(self, value, fill=()):
        size, half = self.size, self.size // 2
        fill = dict(enumerate(fill))
        pieces = [None] * size
        pieces[0] = value
        right = left = value
        for step in range(1, half):
            right, left = self.both(right, left, fill.get(step - 1, ()))
            pieces[size - step] = right
            pieces[step] = left
        rows = value.shape[0] // 2
        pieces[half] = jnp.concatenate(
            self.both(right[:rows], left[rows:], fill.get(half - 1, ())), axis=0
        )
        return pieces

    def scatter_sum(self, lower, upper, fill=()):
        size, half = self.size, self.size // 2
        fill = dict(enumerate(fill))
        rows = lower.shape[0] // size

        def part(ahead, source):
            return source[ahead * rows : (ahead + 1) * rows]

        def whole(ahead):
            return jnp.concatenate([part(ahead, lower), part(ahead, upper)], axis=1)

        right, left = self.both(
            part(half, lower).astype(BF16), part(half, upper).astype(BF16), fill.get(0, ())
        )
        for step in range(1, half):
            if step == 1:
                right = jnp.concatenate(
                    [part(half - 1, lower) + right.astype(F32), part(half - 1, upper)], axis=1
                )
                left = jnp.concatenate(
                    [part(half + 1, lower), part(half + 1, upper) + left.astype(F32)], axis=1
                )
            else:
                right = whole(half - step) + right.astype(F32)
                left = whole(half + step) + left.astype(F32)
            right, left = self.both(
                right.astype(BF16), left.astype(BF16), fill.get(step, ())
            )
        if half == 1:
            return jnp.concatenate(
                [part(0, lower) + right.astype(F32), part(0, upper) + left.astype(F32)], axis=1
            )
        return whole(0) + right.astype(F32) + left.astype(F32)


def column_blocks(weight, size):
    width = weight.shape[1] // size
    return jnp.stack([weight[:, i * width : (i + 1) * width] for i in range(size)])


def join_columns(stacked):
    return jnp.concatenate([stacked[i] for i in range(stacked.shape[0])], axis=1)


def swap_halves(values, half):
    width = values.shape[-1]
    if width == 2 * half:
        return jnp.concatenate([values[:, half:], values[:, :half]], axis=1)
    lane = lax.broadcasted_iota(jnp.int32, values.shape, 1)
    ahead = pltpu.roll(values, width - half, 1)
    behind = pltpu.roll(values, half, 1)
    return jnp.where(lax.rem(lane, 2 * half) < half, ahead, behind)


def head_only(values, lane, head, head_size):
    inside = (lane >= head * head_size) & (lane < (head + 1) * head_size)
    return jnp.where(inside, values, jnp.zeros_like(values))


def flat(ref):
    value = ref[...]
    return value.reshape((value.shape[0] * value.shape[1], value.shape[2]))


def forward_kernel(
    head_size, lengths_ref, q_ref, k_ref, v_ref, cq_ref, sq_ref, ck_ref, sk_ref, qp_ref, kp_ref,
    out_ref, qr_ref, kr_ref, vr_ref, lse_ref,
):
    length = lengths_ref[pl.program_id(0)]
    half = head_size // 2
    queries = flat(q_ref)
    keys = flat(k_ref)
    queries = (queries * cq_ref[...] + swap_halves(queries, half) * sq_ref[...]).astype(BF16)
    keys = (keys * ck_ref[...] + swap_halves(keys, half) * sk_ref[...]).astype(BF16)
    values = flat(v_ref).astype(BF16)
    qr_ref[...] = queries.reshape(qr_ref.shape)
    kr_ref[...] = keys.reshape(kr_ref.shape)
    vr_ref[...] = values.reshape(vr_ref.shape)
    rows, width = queries.shape
    lane = lax.broadcasted_iota(jnp.int32, (rows, width), 1)
    query_pos = qp_ref[:, 0:1]
    key_pos = kp_ref[0:1, :]
    allowed = (key_pos <= query_pos) & (key_pos < length)
    total = jnp.zeros((rows, width), F32)
    scale = head_size ** (-0.5)
    for head in range(width // head_size):
        one = head_only(queries, lane, head, head_size)
        scores = contract(one, keys, 1, 1) * scale
        masked = jnp.where(allowed, scores, NEGATIVE)
        peak = jnp.max(masked, axis=-1, keepdims=True)
        weights = jnp.where(allowed, jnp.exp(masked - peak), 0.0)
        mass = jnp.sum(weights, axis=-1, keepdims=True)
        lse_ref[:, head : head + 1] = peak + jnp.log(mass)
        mixed = contract(weights.astype(BF16), values, 1, 0) / mass
        total = total + head_only(mixed, lane, head, head_size)
    out_ref[...] = total.astype(BF16).reshape(out_ref.shape)


def backward_kernel(
    head_size, lengths_ref, q_ref, k_ref, v_ref, g_ref, lse_ref, cq_ref, sq_ref, ck_ref, sk_ref, qp_ref,
    kp_ref, dq_ref, dk_ref, dv_ref, dk_sum, dv_sum,
):
    length = lengths_ref[pl.program_id(0)]
    half = head_size // 2
    queries, keys, values, grads = flat(q_ref), flat(k_ref), flat(v_ref), flat(g_ref)
    rows, width = queries.shape
    lane = lax.broadcasted_iota(jnp.int32, (rows, width), 1)
    allowed = (kp_ref[0:1, :] <= qp_ref[:, 0:1]) & (kp_ref[0:1, :] < length)
    scale = head_size ** (-0.5)

    @pl.when(pl.program_id(1) == 0)
    def start():
        dk_sum[...] = jnp.zeros_like(dk_sum)
        dv_sum[...] = jnp.zeros_like(dv_sum)

    dq = jnp.zeros((rows, width), F32)
    for head in range(width // head_size):
        one = head_only(queries, lane, head, head_size)
        grad = head_only(grads, lane, head, head_size)
        scores = contract(one, keys, 1, 1) * scale
        prob = jnp.where(
            allowed,
            jnp.exp(jnp.where(allowed, scores, NEGATIVE) - lse_ref[:, head : head + 1]),
            0.0,
        )
        grad_prob = contract(grad, values, 1, 1)
        delta = jnp.sum(prob * grad_prob, axis=-1, keepdims=True)
        grad_score = (prob * (grad_prob - delta) * scale).astype(BF16)
        dq = dq + head_only(contract(grad_score, keys, 1, 0), lane, head, head_size)
        dk_sum[...] += contract(grad_score, one, 0, 0)
        dv_sum[...] += contract(prob.astype(BF16), grad, 0, 0)
    dq = dq * cq_ref[...] - swap_halves(dq, half) * sq_ref[...]
    dq_ref[...] = dq.astype(BF16).reshape(dq_ref.shape)

    @pl.when(pl.program_id(1) == pl.num_programs(1) - 1)
    def finish():
        dk = dk_sum[...]
        dk = dk * ck_ref[...] - swap_halves(dk, half) * sk_ref[...]
        dk_ref[...] = dk.astype(BF16).reshape(dk_ref.shape)
        dv_ref[...] = dv_sum[...].astype(BF16).reshape(dv_ref.shape)


class Attention:
    def __init__(self, size, groups, slots, width, head_size, lengths, owners):
        self.size, self.groups, self.slots, self.width = size, groups, slots, width
        self.head_size = head_size
        self.lengths = lengths
        self.heads = width // head_size
        self.steps = max(1, min(size, QUERY_ROWS // slots))
        half = head_size // 2
        positions = (owners[:, None] * slots + jnp.arange(slots, dtype=jnp.int32)[None]).reshape(-1)
        freqs = THETA ** (-(jnp.arange(half, dtype=F32) * 2.0) / (2.0 * half))
        angles = positions.astype(F32)[:, None] * freqs[None, :]
        cosine, sine = jnp.cos(angles), jnp.sin(angles)
        self.cosine = jnp.tile(cosine, (1, 2 * self.heads))
        self.sine = jnp.tile(jnp.concatenate([-sine, sine], axis=1), (1, self.heads))
        self.query_pos = jnp.broadcast_to(positions[:, None], (positions.shape[0], 128))
        self.key_pos = jnp.broadcast_to(positions[None, :], (8, positions.shape[0]))
        total = size * slots
        rows = self.steps * slots
        self.grid = (groups, size // self.steps)
        self.q_spec = self.tokens(self.steps, width, 0, True)
        self.k_spec = self.tokens(size, width, 0, False)
        self.table_q = pl.BlockSpec((rows, width), lambda b, i, *_: (i, 0))
        self.table_k = pl.BlockSpec((total, width), lambda b, i, *_: (0, 0))
        self.pos_q = pl.BlockSpec((rows, 128), lambda b, i, *_: (i, 0))
        self.pos_k = pl.BlockSpec((8, total), lambda b, i, *_: (0, 0))
        self.lse = pl.BlockSpec((None, rows, self.heads), lambda b, i, *_: (b, i, 0))
        self.lse_shape = jax.ShapeDtypeStruct((groups, total, self.heads), F32)
        self.shape = jax.ShapeDtypeStruct((size, groups, slots, width), BF16)
        self.work = groups * self.heads * total * total

    def tokens(self, count, width, column, moving):
        return pl.BlockSpec(
            (count, None, self.slots, width),
            (lambda b, i, *_: (i, b, 0, column)) if moving else (lambda b, i, *_: (0, b, 0, column)),
        )

    def split(self, array):
        return array.reshape(self.size, self.groups, self.slots, -1)

    def cost(self, matmuls):
        return pl.CostEstimate(
            flops=2 * matmuls * self.work * self.head_size,
            transcendentals=self.work,
            bytes_accessed=8 * self.size * self.groups * self.slots * self.width * 2,
        )

    def forward(self, projected):
        width = self.width
        if width % 128 == 0:
            arrays = (self.split(projected),) * 3
            columns = (0, 1, 2)
        else:
            arrays = tuple(
                self.split(projected[:, i * width : (i + 1) * width]) for i in range(3)
            )
            columns = (0, 0, 0)
        return pl.pallas_call(
            functools.partial(forward_kernel, self.head_size),
            grid_spec=pltpu.PrefetchScalarGridSpec(
                num_scalar_prefetch=1,
                grid=self.grid,
                in_specs=[
                    self.tokens(self.steps, width, columns[0], True),
                    self.tokens(self.size, width, columns[1], False),
                    self.tokens(self.size, width, columns[2], False),
                    self.table_q, self.table_q, self.table_k, self.table_k, self.pos_q, self.pos_k,
                ],
                out_specs=[self.q_spec, self.q_spec, self.k_spec, self.k_spec, self.lse],
            ),
            out_shape=[self.shape] * 4 + [self.lse_shape],
            cost_estimate=self.cost(2),
            name="attention_forward",
        )(
            self.lengths, *arrays, self.cosine, self.sine, self.cosine, self.sine, self.query_pos, self.key_pos
        )

    def backward(self, queries, keys, values, grads, lse):
        total = self.size * self.slots
        return pl.pallas_call(
            functools.partial(backward_kernel, self.head_size),
            grid_spec=pltpu.PrefetchScalarGridSpec(
                num_scalar_prefetch=1,
                grid=self.grid,
                in_specs=[
                    self.q_spec, self.k_spec, self.k_spec, self.q_spec, self.lse,
                    self.table_q, self.table_q, self.table_k, self.table_k, self.pos_q, self.pos_k,
                ],
                out_specs=[self.q_spec, self.k_spec, self.k_spec],
                scratch_shapes=[pltpu.VMEM((total, self.width), F32)] * 2,
            ),
            out_shape=[self.shape] * 3,
            cost_estimate=self.cost(5),
            name="attention_backward",
        )(
            self.lengths, queries, keys, values, self.split(grads), lse,
            self.cosine, self.sine, self.cosine, self.sine, self.query_pos, self.key_pos,
        )


def body(
    inputs, cotangent, lengths, query_weight, key_weight, value_weight, mix_weight, gate_weight,
    up_weight, down_weight, attn_gain, ffn_gain,
):
    groups, slots, width = inputs.shape
    head_size = width // HEADS
    size = lax.axis_size("ctx")
    count = lax.axis_size("dp")
    rows = groups * slots
    ring = Ring(size)
    shares = Shares(count)
    owners = ring.owners()
    local = width // size
    hidden_local = gate_weight.shape[1] // size
    gain_one = attn_gain.astype(F32)[:, None]
    gain_two = ffn_gain.astype(F32)[:, None]

    def scaled(weight, gain):
        return (weight.astype(F32) * gain).astype(BF16)

    def exchange(blocks, done=()):
        return lax.all_to_all(tie([blocks], done)[0], "ctx", 0, 0, tiled=True)

    def to_columns(weights, done=()):
        blocks = jnp.concatenate([column_blocks(w, size) for w in weights], axis=2)
        return exchange(blocks, done).reshape(-1, blocks.shape[2])

    def to_rows(total, done=()):
        return exchange(total.reshape(size, -1, total.shape[1]), done)

    def halves(pieces):
        half = width // 2
        return (
            jnp.concatenate([p[:, :half] for p in pieces], axis=0),
            jnp.concatenate([p[:, half:] for p in pieces], axis=0),
        )

    def apply(values, weights):
        return contract(values[0], weights[0], 1, 0) + contract(values[1], weights[1], 1, 0)

    block_in = shares.to_order(inputs.reshape(rows, width)).astype(F32)
    positions = lax.axis_index("ctx") * slots + jnp.arange(slots, dtype=jnp.int32)
    valid = (positions[None, :] < lengths[:, None]).astype(F32).reshape(rows, 1)
    normed_one, factor_one = normalize(block_in)
    grad_out = shares.to_order(cotangent.reshape(rows, width)).astype(F32) * valid

    to_shares = [(i * size + j, j * count + i) for i in range(count) for j in range(size)]
    from_shares = [(there, here) for here, there in to_shares]
    attn_columns = to_columns([scaled(w, gain_one) for w in (query_weight, key_weight, value_weight)])
    one_all = halves(ring.gather(normed_one.astype(BF16)))
    mix_share = lax.ppermute(tie([mix_weight], ring.steps[-2])[0], ("dp", "ctx"), from_shares)
    attn_weights = shares.gather(attn_columns)
    projected = apply(one_all, attn_weights)
    ffn_columns = to_columns(
        [scaled(gate_weight, gain_two), scaled(up_weight, gain_two), down_weight], ring.done
    )
    ffn_half = shares.gather_far(ffn_columns[:, : 2 * hidden_local])
    down_half = shares.gather_far(ffn_columns[:, 2 * hidden_local :], (ffn_half,))
    attention = Attention(size, groups, slots, local, head_size, lengths, owners)
    mixed, query_rot, key_rot, value_low, lse = attention.forward(projected)
    mixed = mixed.reshape(size * rows, local)
    mix_parts = shares.gather(mix_share, (mixed,))
    mix_blocks = jnp.split(jnp.concatenate(mix_parts, axis=0), count, axis=0)
    mix_rows = shares.to_order(
        jnp.concatenate(
            shares.relative([mix_blocks[shares.order.index(k)] for k in range(count)]), axis=0
        )
    )
    attn_out = contract(mixed, mix_rows, 1, 0)
    residual = block_in + ring.scatter_sum(
        attn_out[:, : width // 2], attn_out[:, width // 2 :], ((ffn_columns,),)
    )

    ffn_weights = (ffn_half, shares.swap(ffn_half, 1))
    normed_two, factor_two = normalize(residual)
    two_all = halves(ring.gather(normed_two.astype(BF16), ((), (ffn_half,))))
    down_weights = (down_half, shares.swap(down_half, 1))
    low_part = contract(two_all[0], ffn_weights[0], 1, 0)
    gate_up = low_part + contract(two_all[1], ffn_weights[1], 1, 0)
    gate, up = gate_up[:, :hidden_local], gate_up[:, hidden_local:]
    sigma = jax.nn.sigmoid(gate)
    silu_gate = gate * sigma
    hidden = (silu_gate * up).astype(BF16)
    grad_all = halves(
        ring.gather(grad_out.astype(BF16), fill=((), (low_part, down_half), (gate_up,), (hidden,)))
    )
    branch = ring.scatter_sum(*(contract(hidden, w, 1, 1) for w in down_weights))
    activations = valid * (residual + branch)

    grad_hidden = apply(grad_all, down_weights)
    grad_both = jnp.concatenate(
        [
            (grad_hidden * up * sigma * (1.0 + gate * (1.0 - sigma))).astype(BF16),
            (grad_hidden * silu_gate).astype(BF16),
        ],
        axis=1,
    )

    def summed(values, gradient):
        given = contract(values[1], gradient, 0, 0).astype(BF16)
        return given, shares.scatter_core(contract(values[0], gradient, 0, 0), given)

    down_given, down_half = summed(grad_all, hidden)
    both_given, both_half = summed(two_all, grad_both)
    down_sum = shares.scatter_rest(down_half)
    both_sum = shares.scatter_rest(tie([both_half], (down_sum,))[0])
    scaled_two = ring.scatter_sum(
        *(contract(grad_both, w, 1, 1) for w in ffn_weights),
        fill=((), (down_given,), (both_given,), (down_half,)),
    )
    dres = grad_out + factor_two * (
        scaled_two - normed_two * jnp.mean(normed_two * scaled_two, axis=-1, keepdims=True)
    )
    dres_low = dres.astype(BF16)

    dres_pieces = ring.gather(dres_low, fill=((both_half,),))
    dres_all = jnp.concatenate(dres_pieces, axis=0)
    down_rows = to_rows(down_sum, ring.steps[-2])
    both_rows = to_rows(both_sum, ring.steps[-2])
    grad_heads = contract(dres_all, mix_rows, 1, 1).astype(BF16)
    dq, dk, dv = attention.backward(
        query_rot, key_rot, value_low, *tie([grad_heads], (both_sum, down_rows)), lse
    )
    projected_grad = jnp.concatenate(
        [d.reshape(size * rows, local) for d in (dq, dk, dv)], axis=1
    )
    (projected_grad,) = tie([projected_grad], (both_rows,))
    attn_given, attn_half = summed(one_all, projected_grad)
    attn_rows = to_rows(shares.scatter_rest(attn_half))
    mix_terms = shares.from_order(contract(mixed, dres_all, 0, 0))
    mix_blocks = shares.relative(jnp.split(mix_terms, count, axis=0))
    mix_blocks = [mix_blocks[k] for k in shares.order]
    mix_given = jnp.concatenate(mix_blocks[count // 2 :], axis=0).astype(BF16)
    mix_sum = shares.scatter_rest(
        shares.scatter_core(jnp.concatenate(mix_blocks[: count // 2], axis=0), mix_given)
    )
    scaled_one = ring.scatter_sum(
        *(contract(projected_grad, w, 1, 1) for w in attn_weights),
        fill=((attn_given,), (attn_half,), (), (attn_rows,)),
    )
    input_grad = dres + factor_one * (
        scaled_one - normed_one * jnp.mean(normed_one * scaled_one, axis=-1, keepdims=True)
    )
    (mix_sum,) = tie([mix_sum], ring.steps[-2])
    mix_grad = lax.ppermute(mix_sum, ("dp", "ctx"), to_shares).astype(F32)

    def joined(rows, columns):
        return join_columns(rows[:, :, columns]).astype(F32)

    down_grad = joined(down_rows, slice(None))
    gate_raw = joined(both_rows, slice(0, hidden_local))
    up_raw = joined(both_rows, slice(hidden_local, 2 * hidden_local))
    query_raw, key_raw, value_raw = (
        joined(attn_rows, slice(i * local, (i + 1) * local)) for i in range(3)
    )

    def row_sum(*pairs):
        return sum(jnp.sum(w.astype(F32) * g, axis=1) for w, g in pairs)

    attn_gain_grad = row_sum(
        (query_weight, query_raw), (key_weight, key_raw), (value_weight, value_raw)
    )
    ffn_gain_grad = row_sum((gate_weight, gate_raw), (up_weight, up_raw))
    return (
        shares.from_order(activations.astype(BF16)).reshape(groups, slots, width),
        shares.from_order(input_grad.astype(BF16)).reshape(groups, slots, width),
        query_raw * gain_one,
        key_raw * gain_one,
        value_raw * gain_one,
        mix_grad,
        gate_raw * gain_two,
        up_raw * gain_two,
        down_grad,
        attn_gain_grad,
        ffn_gain_grad,
    )


def solution(mesh):
    rows = P(("dp", "ctx"), None)
    tokens = P("dp", "ctx", None)
    gains = P(("dp", "ctx"))
    return jax.shard_map(
        body,
        mesh=mesh,
        in_specs=(tokens, tokens, P("dp")) + (rows,) * 7 + (gains, gains),
        out_specs=(tokens, tokens) + (rows,) * 7 + (gains, gains),
        check_vma=False,
    )
```

```python
import functools

import jax
import jax.numpy as jnp
from jax import lax
from jax.experimental import pallas as pl
from jax.experimental.pallas import tpu as pltpu
from jax.sharding import PartitionSpec as P

HEADS = 32
EPSILON = 1e-05
THETA = 130000.0
NEGATIVE = -1e30
QUERY_ROWS = 512
BF16 = jnp.bfloat16
F32 = jnp.float32


def normalize(values):
    factor = lax.rsqrt(jnp.mean(values * values, axis=-1, keepdims=True) + EPSILON)
    return (values * factor, factor)


def contract(left, right, left_dim, right_dim):
    return lax.dot_general(
        left, right, (((left_dim,), (right_dim,)), ((), ())), preferred_element_type=F32
    )


def tie(values, done):
    done = tuple(done)
    if not done:
        return list(values)
    return list(lax.optimization_barrier((tuple(values), done))[0])


class Shares:
    def __init__(self, count):
        self.count = count
        self.index = lax.axis_index("dp")
        self.bits = [1 << i for i in range(count.bit_length() - 1)]
        even = [0]
        for bit in self.bits[1:]:
            even = even + [k ^ bit for k in even]
        self.order = even + [k ^ 1 for k in even] if count > 1 else even

    def swap(self, value, bit):
        return lax.ppermute(value, "dp", [(i, i ^ bit) for i in range(self.count)])

    def relative(self, blocks):
        for bit in self.bits:
            odd = (self.index & bit) != 0
            blocks = [jnp.where(odd, blocks[k ^ bit], blocks[k]) for k in range(self.count)]
        return blocks

    def to_order(self, values):
        blocks = self.relative(jnp.split(values, self.count, axis=1))
        return jnp.concatenate([blocks[k] for k in self.order], axis=1)

    def from_order(self, values):
        parts = jnp.split(values, self.count, axis=1)
        blocks = [parts[self.order.index(k)] for k in range(self.count)]
        return jnp.concatenate(self.relative(blocks), axis=1)

    def gather_far(self, block, done=()):
        (value,) = tie([block], done)
        for bit in self.bits[1:]:
            value = jnp.concatenate([value, self.swap(value, bit)], axis=0)
        return value

    def gather(self, block, done=()):
        value = self.gather_far(block, done)
        return value, self.swap(value, 1)

    def scatter_core(self, kept, given):
        return kept + self.swap(given, 1).astype(F32)

    def scatter_rest(self, total):
        for bit in reversed(self.bits[1:]):
            half = total.shape[0] // 2
            low = total[half:].astype(BF16)
            total = total[:half] + self.swap(low, bit).astype(F32)
        return total.astype(BF16)


class Ring:
    def __init__(self, size):
        self.size = size
        self.order = list(range(0, size, 2)) + list(range(size - 1, 0, -2))
        index = lax.axis_index("ctx")
        self.place = jnp.where(index % 2 == 0, index // 2, size - (index + 1) // 2)
        self.done = ()
        self.steps = []

    def owner(self, ahead):
        place = lax.rem(self.place + ahead, self.size)
        return jnp.where(place < self.size // 2, 2 * place, 2 * (self.size - place) - 1)

    def owners(self):
        return self.owner(jnp.arange(self.size, dtype=jnp.int32))

    def shift(self, value, by):
        pairs = [
            (self.order[i], self.order[(i + by) % self.size]) for i in range(self.size)
        ]
        return lax.ppermute(value, "ctx", pairs)

    def both(self, right, left, done=()):
        right, left = tie((right, left), (*self.done, *done))
        right, left = self.shift(right, 1), self.shift(left, -1)
        self.done = (right, left)
        self.steps.append(self.done)
        return right, left

    def gather(self, value, fill=()):
        size, half = self.size, self.size // 2
        fill = dict(enumerate(fill))
        pieces = [None] * size
        pieces[0] = value
        right = left = value
        for step in range(1, half):
            right, left = self.both(right, left, fill.get(step - 1, ()))
            pieces[size - step] = right
            pieces[step] = left
        rows = value.shape[0] // 2
        pieces[half] = jnp.concatenate(
            self.both(right[:rows], left[rows:], fill.get(half - 1, ())), axis=0
        )
        return pieces

    def scatter_sum(self, lower, upper, fill=()):
        size, half = self.size, self.size // 2
        fill = dict(enumerate(fill))
        rows = lower.shape[0] // size

        def part(ahead, source):
            return source[ahead * rows : (ahead + 1) * rows]

        def whole(ahead):
            return jnp.concatenate([part(ahead, lower), part(ahead, upper)], axis=1)

        right, left = self.both(
            part(half, lower).astype(BF16), part(half, upper).astype(BF16), fill.get(0, ())
        )
        for step in range(1, half):
            if step == 1:
                right = jnp.concatenate(
                    [part(half - 1, lower) + right.astype(F32), part(half - 1, upper)], axis=1
                )
                left = jnp.concatenate(
                    [part(half + 1, lower), part(half + 1, upper) + left.astype(F32)], axis=1
                )
            else:
                right = whole(half - step) + right.astype(F32)
                left = whole(half + step) + left.astype(F32)
            right, left = self.both(
                right.astype(BF16), left.astype(BF16), fill.get(step, ())
            )
        if half == 1:
            return jnp.concatenate(
                [part(0, lower) + right.astype(F32), part(0, upper) + left.astype(F32)], axis=1
            )
        return whole(0) + right.astype(F32) + left.astype(F32)


def column_blocks(weight, size):
    width = weight.shape[1] // size
    return jnp.stack([weight[:, i * width : (i + 1) * width] for i in range(size)])


def join_columns(stacked):
    return jnp.concatenate([stacked[i] for i in range(stacked.shape[0])], axis=1)


def swap_halves(values, half):
    width = values.shape[-1]
    if width == 2 * half:
        return jnp.concatenate([values[:, half:], values[:, :half]], axis=1)
    lane = lax.broadcasted_iota(jnp.int32, values.shape, 1)
    ahead = pltpu.roll(values, width - half, 1)
    behind = pltpu.roll(values, half, 1)
    return jnp.where(lax.rem(lane, 2 * half) < half, ahead, behind)


def head_only(values, lane, head, head_size):
    inside = (lane >= head * head_size) & (lane < (head + 1) * head_size)
    return jnp.where(inside, values, jnp.zeros_like(values))


def flat(ref):
    value = ref[...]
    return value.reshape((value.shape[0] * value.shape[1], value.shape[2]))


def forward_kernel(
    head_size, lengths_ref, q_ref, k_ref, v_ref, cq_ref, sq_ref, ck_ref, sk_ref, qp_ref, kp_ref,
    out_ref, qr_ref, kr_ref, vr_ref, lse_ref,
):
    length = lengths_ref[pl.program_id(0)]
    half = head_size // 2
    queries = flat(q_ref)
    keys = flat(k_ref)
    queries = (queries * cq_ref[...] + swap_halves(queries, half) * sq_ref[...]).astype(BF16)
    keys = (keys * ck_ref[...] + swap_halves(keys, half) * sk_ref[...]).astype(BF16)
    values = flat(v_ref).astype(BF16)
    qr_ref[...] = queries.reshape(qr_ref.shape)
    kr_ref[...] = keys.reshape(kr_ref.shape)
    vr_ref[...] = values.reshape(vr_ref.shape)
    rows, width = queries.shape
    lane = lax.broadcasted_iota(jnp.int32, (rows, width), 1)
    query_pos = qp_ref[:, 0:1]
    key_pos = kp_ref[0:1, :]
    allowed = (key_pos <= query_pos) & (key_pos < length)
    total = jnp.zeros((rows, width), F32)
    scale = head_size ** (-0.5)
    for head in range(width // head_size):
        one = head_only(queries, lane, head, head_size)
        scores = contract(one, keys, 1, 1) * scale
        masked = jnp.where(allowed, scores, NEGATIVE)
        peak = jnp.max(masked, axis=-1, keepdims=True)
        weights = jnp.where(allowed, jnp.exp(masked - peak), 0.0)
        mass = jnp.sum(weights, axis=-1, keepdims=True)
        lse_ref[:, head : head + 1] = peak + jnp.log(mass)
        mixed = contract(weights.astype(BF16), values, 1, 0) / mass
        total = total + head_only(mixed, lane, head, head_size)
    out_ref[...] = total.astype(BF16).reshape(out_ref.shape)


def backward_kernel(
    head_size, lengths_ref, q_ref, k_ref, v_ref, g_ref, lse_ref, cq_ref, sq_ref, ck_ref, sk_ref, qp_ref,
    kp_ref, dq_ref, dk_ref, dv_ref, dk_sum, dv_sum,
):
    length = lengths_ref[pl.program_id(0)]
    half = head_size // 2
    queries, keys, values, grads = flat(q_ref), flat(k_ref), flat(v_ref), flat(g_ref)
    rows, width = queries.shape
    lane = lax.broadcasted_iota(jnp.int32, (rows, width), 1)
    allowed = (kp_ref[0:1, :] <= qp_ref[:, 0:1]) & (kp_ref[0:1, :] < length)
    scale = head_size ** (-0.5)

    @pl.when(pl.program_id(1) == 0)
    def start():
        dk_sum[...] = jnp.zeros_like(dk_sum)
        dv_sum[...] = jnp.zeros_like(dv_sum)

    dq = jnp.zeros((rows, width), F32)
    for head in range(width // head_size):
        one = head_only(queries, lane, head, head_size)
        grad = head_only(grads, lane, head, head_size)
        scores = contract(one, keys, 1, 1) * scale
        prob = jnp.where(
            allowed,
            jnp.exp(jnp.where(allowed, scores, NEGATIVE) - lse_ref[:, head : head + 1]),
            0.0,
        )
        grad_prob = contract(grad, values, 1, 1)
        delta = jnp.sum(prob * grad_prob, axis=-1, keepdims=True)
        grad_score = (prob * (grad_prob - delta) * scale).astype(BF16)
        dq = dq + head_only(contract(grad_score, keys, 1, 0), lane, head, head_size)
        dk_sum[...] += contract(grad_score, one, 0, 0)
        dv_sum[...] += contract(prob.astype(BF16), grad, 0, 0)
    dq = dq * cq_ref[...] - swap_halves(dq, half) * sq_ref[...]
    dq_ref[...] = dq.astype(BF16).reshape(dq_ref.shape)

    @pl.when(pl.program_id(1) == pl.num_programs(1) - 1)
    def finish():
        dk = dk_sum[...]
        dk = dk * ck_ref[...] - swap_halves(dk, half) * sk_ref[...]
        dk_ref[...] = dk.astype(BF16).reshape(dk_ref.shape)
        dv_ref[...] = dv_sum[...].astype(BF16).reshape(dv_ref.shape)


class Attention:
    def __init__(self, size, groups, slots, width, head_size, lengths, owners):
        self.size, self.groups, self.slots, self.width = size, groups, slots, width
        self.head_size = head_size
        self.lengths = lengths
        self.heads = width // head_size
        self.steps = max(1, min(size, QUERY_ROWS // slots))
        half = head_size // 2
        positions = (owners[:, None] * slots + jnp.arange(slots, dtype=jnp.int32)[None]).reshape(-1)
        freqs = THETA ** (-(jnp.arange(half, dtype=F32) * 2.0) / (2.0 * half))
        angles = positions.astype(F32)[:, None] * freqs[None, :]
        cosine, sine = jnp.cos(angles), jnp.sin(angles)
        self.cosine = jnp.tile(cosine, (1, 2 * self.heads))
        self.sine = jnp.tile(jnp.concatenate([-sine, sine], axis=1), (1, self.heads))
        self.query_pos = jnp.broadcast_to(positions[:, None], (positions.shape[0], 128))
        self.key_pos = jnp.broadcast_to(positions[None, :], (8, positions.shape[0]))
        total = size * slots
        rows = self.steps * slots
        self.grid = (groups, size // self.steps)
        self.q_spec = self.tokens(self.steps, width, 0, True)
        self.k_spec = self.tokens(size, width, 0, False)
        self.table_q = pl.BlockSpec((rows, width), lambda b, i, *_: (i, 0))
        self.table_k = pl.BlockSpec((total, width), lambda b, i, *_: (0, 0))
        self.pos_q = pl.BlockSpec((rows, 128), lambda b, i, *_: (i, 0))
        self.pos_k = pl.BlockSpec((8, total), lambda b, i, *_: (0, 0))
        self.lse = pl.BlockSpec((None, rows, self.heads), lambda b, i, *_: (b, i, 0))
        self.lse_shape = jax.ShapeDtypeStruct((groups, total, self.heads), F32)
        self.shape = jax.ShapeDtypeStruct((size, groups, slots, width), BF16)
        self.work = groups * self.heads * total * total

    def tokens(self, count, width, column, moving):
        return pl.BlockSpec(
            (count, None, self.slots, width),
            (lambda b, i, *_: (i, b, 0, column)) if moving else (lambda b, i, *_: (0, b, 0, column)),
        )

    def split(self, array):
        return array.reshape(self.size, self.groups, self.slots, -1)

    def cost(self, matmuls):
        return pl.CostEstimate(
            flops=2 * matmuls * self.work * self.head_size,
            transcendentals=self.work,
            bytes_accessed=8 * self.size * self.groups * self.slots * self.width * 2,
        )

    def forward(self, projected):
        width = self.width
        if width % 128 == 0:
            arrays = (self.split(projected),) * 3
            columns = (0, 1, 2)
        else:
            arrays = tuple(
                self.split(projected[:, i * width : (i + 1) * width]) for i in range(3)
            )
            columns = (0, 0, 0)
        return pl.pallas_call(
            functools.partial(forward_kernel, self.head_size),
            grid_spec=pltpu.PrefetchScalarGridSpec(
                num_scalar_prefetch=1,
                grid=self.grid,
                in_specs=[
                    self.tokens(self.steps, width, columns[0], True),
                    self.tokens(self.size, width, columns[1], False),
                    self.tokens(self.size, width, columns[2], False),
                    self.table_q, self.table_q, self.table_k, self.table_k, self.pos_q, self.pos_k,
                ],
                out_specs=[self.q_spec, self.q_spec, self.k_spec, self.k_spec, self.lse],
            ),
            out_shape=[self.shape] * 4 + [self.lse_shape],
            cost_estimate=self.cost(2),
            name="attention_forward",
        )(
            self.lengths, *arrays, self.cosine, self.sine, self.cosine, self.sine, self.query_pos, self.key_pos
        )

    def backward(self, queries, keys, values, grads, lse):
        total = self.size * self.slots
        return pl.pallas_call(
            functools.partial(backward_kernel, self.head_size),
            grid_spec=pltpu.PrefetchScalarGridSpec(
                num_scalar_prefetch=1,
                grid=self.grid,
                in_specs=[
                    self.q_spec, self.k_spec, self.k_spec, self.q_spec, self.lse,
                    self.table_q, self.table_q, self.table_k, self.table_k, self.pos_q, self.pos_k,
                ],
                out_specs=[self.q_spec, self.k_spec, self.k_spec],
                scratch_shapes=[pltpu.VMEM((total, self.width), F32)] * 2,
            ),
            out_shape=[self.shape] * 3,
            cost_estimate=self.cost(5),
            name="attention_backward",
        )(
            self.lengths, queries, keys, values, self.split(grads), lse,
            self.cosine, self.sine, self.cosine, self.sine, self.query_pos, self.key_pos,
        )


def body(
    inputs, cotangent, lengths, query_weight, key_weight, value_weight, mix_weight, gate_weight,
    up_weight, down_weight, attn_gain, ffn_gain,
):
    groups, slots, width = inputs.shape
    head_size = width // HEADS
    size = lax.axis_size("ctx")
    count = lax.axis_size("dp")
    rows = groups * slots
    ring = Ring(size)
    shares = Shares(count)
    owners = ring.owners()
    local = width // size
    hidden_local = gate_weight.shape[1] // size
    gain_one = attn_gain.astype(F32)[:, None]
    gain_two = ffn_gain.astype(F32)[:, None]

    def scaled(weight, gain):
        return (weight.astype(F32) * gain).astype(BF16)

    def exchange(blocks, done=()):
        return lax.all_to_all(tie([blocks], done)[0], "ctx", 0, 0, tiled=True)

    def to_columns(weights, done=()):
        blocks = jnp.concatenate([column_blocks(w, size) for w in weights], axis=2)
        return exchange(blocks, done).reshape(-1, blocks.shape[2])

    def to_rows(total, done=()):
        return exchange(total.reshape(size, -1, total.shape[1]), done)

    def halves(pieces):
        half = width // 2
        return (
            jnp.concatenate([p[:, :half] for p in pieces], axis=0),
            jnp.concatenate([p[:, half:] for p in pieces], axis=0),
        )

    def apply(values, weights):
        return contract(values[0], weights[0], 1, 0) + contract(values[1], weights[1], 1, 0)

    block_in = shares.to_order(inputs.reshape(rows, width)).astype(F32)
    positions = lax.axis_index("ctx") * slots + jnp.arange(slots, dtype=jnp.int32)
    valid = (positions[None, :] < lengths[:, None]).astype(F32).reshape(rows, 1)
    normed_one, factor_one = normalize(block_in)
    grad_out = shares.to_order(cotangent.reshape(rows, width)).astype(F32) * valid

    to_shares = [(i * size + j, j * count + i) for i in range(count) for j in range(size)]
    from_shares = [(there, here) for here, there in to_shares]
    attn_columns = to_columns([scaled(w, gain_one) for w in (query_weight, key_weight, value_weight)])
    one_all = halves(ring.gather(normed_one.astype(BF16)))
    mix_share = lax.ppermute(tie([mix_weight], ring.steps[-2])[0], ("dp", "ctx"), from_shares)
    attn_weights = shares.gather(attn_columns)
    projected = apply(one_all, attn_weights)
    ffn_columns = to_columns(
        [scaled(gate_weight, gain_two), scaled(up_weight, gain_two), down_weight], ring.done
    )
    ffn_parts = []
    for part in jnp.split(ffn_columns, 6, axis=1):
        ffn_parts.append(shares.gather_far(part, ffn_parts[-1:]))
    ffn_half = jnp.concatenate(ffn_parts[:4], axis=1)
    down_half = jnp.concatenate(ffn_parts[4:], axis=1)
    attention = Attention(size, groups, slots, local, head_size, lengths, owners)
    mixed, query_rot, key_rot, value_low, lse = attention.forward(projected)
    mixed = mixed.reshape(size * rows, local)
    mix_parts = shares.gather(mix_share, (mixed,))
    mix_blocks = jnp.split(jnp.concatenate(mix_parts, axis=0), count, axis=0)
    mix_rows = shares.to_order(
        jnp.concatenate(
            shares.relative([mix_blocks[shares.order.index(k)] for k in range(count)]), axis=0
        )
    )
    attn_out = contract(mixed, mix_rows, 1, 0)
    residual = block_in + ring.scatter_sum(
        attn_out[:, : width // 2], attn_out[:, width // 2 :], ((ffn_columns,), ffn_parts[:1], ffn_parts[1:2], ffn_parts[2:3])
    )

    ffn_weights = (ffn_half, shares.swap(ffn_half, 1))
    normed_two, factor_two = normalize(residual)
    two_all = halves(ring.gather(normed_two.astype(BF16), (ffn_parts[3:4], (), ffn_parts[4:5], ffn_parts[5:])))
    down_weights = (down_half, shares.swap(down_half, 1))
    low_part = contract(two_all[0], ffn_weights[0], 1, 0)
    gate_up = low_part + contract(two_all[1], ffn_weights[1], 1, 0)
    gate, up = gate_up[:, :hidden_local], gate_up[:, hidden_local:]
    sigma = jax.nn.sigmoid(gate)
    silu_gate = gate * sigma
    hidden = (silu_gate * up).astype(BF16)
    grad_all = halves(
        ring.gather(grad_out.astype(BF16), fill=((), (low_part,), (gate_up,), (hidden,)))
    )
    branch = ring.scatter_sum(*(contract(hidden, w, 1, 1) for w in down_weights))
    activations = valid * (residual + branch)

    grad_hidden = apply(grad_all, down_weights)
    grad_both = jnp.concatenate(
        [
            (grad_hidden * up * sigma * (1.0 + gate * (1.0 - sigma))).astype(BF16),
            (grad_hidden * silu_gate).astype(BF16),
        ],
        axis=1,
    )

    def summed(values, gradient):
        given = contract(values[1], gradient, 0, 0).astype(BF16)
        return given, shares.scatter_core(contract(values[0], gradient, 0, 0), given)

    down_given, down_half = summed(grad_all, hidden)
    both_given, both_half = summed(two_all, grad_both)
    down_sum = shares.scatter_rest(down_half)
    both_sum = shares.scatter_rest(tie([both_half], (down_sum,))[0])
    scaled_two = ring.scatter_sum(
        *(contract(grad_both, w, 1, 1) for w in ffn_weights),
        fill=((), (down_given,), (both_given,), (down_half,)),
    )
    dres = grad_out + factor_two * (
        scaled_two - normed_two * jnp.mean(normed_two * scaled_two, axis=-1, keepdims=True)
    )
    dres_low = dres.astype(BF16)

    dres_pieces = ring.gather(dres_low, fill=((both_half,),))
    dres_all = jnp.concatenate(dres_pieces, axis=0)
    down_rows = to_rows(down_sum, ring.steps[-2])
    both_rows = to_rows(both_sum, ring.steps[-2])
    grad_heads = contract(dres_all, mix_rows, 1, 1).astype(BF16)
    dq, dk, dv = attention.backward(
        query_rot, key_rot, value_low, *tie([grad_heads], (both_sum, down_rows)), lse
    )
    projected_grad = jnp.concatenate(
        [d.reshape(size * rows, local) for d in (dq, dk, dv)], axis=1
    )
    (projected_grad,) = tie([projected_grad], (both_rows,))
    attn_given, attn_half = summed(one_all, projected_grad)
    attn_sum = shares.scatter_rest(attn_half)
    attn_rows = to_rows(attn_sum)
    mix_terms = shares.from_order(contract(mixed, dres_all, 0, 0))
    mix_blocks = shares.relative(jnp.split(mix_terms, count, axis=0))
    mix_blocks = [mix_blocks[k] for k in shares.order]
    mix_given = jnp.concatenate(mix_blocks[count // 2 :], axis=0).astype(BF16)
    mix_sum = shares.scatter_rest(
        shares.scatter_core(jnp.concatenate(mix_blocks[: count // 2], axis=0), mix_given)
    )
    scaled_one = ring.scatter_sum(
        *(contract(projected_grad, w, 1, 1) for w in attn_weights),
        fill=((attn_given,), (attn_half,), (), (attn_sum,)),
    )
    input_grad = dres + factor_one * (
        scaled_one - normed_one * jnp.mean(normed_one * scaled_one, axis=-1, keepdims=True)
    )
    (mix_sum,) = tie([mix_sum], ring.steps[-2])
    mix_grad = lax.ppermute(mix_sum, ("dp", "ctx"), to_shares).astype(F32)

    def joined(rows, columns):
        return join_columns(rows[:, :, columns]).astype(F32)

    down_grad = joined(down_rows, slice(None))
    gate_raw = joined(both_rows, slice(0, hidden_local))
    up_raw = joined(both_rows, slice(hidden_local, 2 * hidden_local))
    query_raw, key_raw, value_raw = (
        joined(attn_rows, slice(i * local, (i + 1) * local)) for i in range(3)
    )

    def row_sum(*pairs):
        return sum(jnp.sum(w.astype(F32) * g, axis=1) for w, g in pairs)

    attn_gain_grad = row_sum(
        (query_weight, query_raw), (key_weight, key_raw), (value_weight, value_raw)
    )
    ffn_gain_grad = row_sum((gate_weight, gate_raw), (up_weight, up_raw))
    return (
        shares.from_order(activations.astype(BF16)).reshape(groups, slots, width),
        shares.from_order(input_grad.astype(BF16)).reshape(groups, slots, width),
        query_raw * gain_one,
        key_raw * gain_one,
        value_raw * gain_one,
        mix_grad,
        gate_raw * gain_two,
        up_raw * gain_two,
        down_grad,
        attn_gain_grad,
        ffn_gain_grad,
    )


def solution(mesh):
    rows = P(("dp", "ctx"), None)
    tokens = P("dp", "ctx", None)
    gains = P(("dp", "ctx"))
    return jax.shard_map(
        body,
        mesh=mesh,
        in_specs=(tokens, tokens, P("dp")) + (rows,) * 7 + (gains, gains),
        out_specs=(tokens, tokens) + (rows,) * 7 + (gains, gains),
        check_vma=False,
    )
```

```python
import functools

import jax
import jax.numpy as jnp
from jax import lax
from jax.experimental import pallas as pl
from jax.experimental.pallas import tpu as pltpu
from jax.sharding import PartitionSpec as P

HEADS = 32
EPSILON = 1e-05
THETA = 130000.0
NEGATIVE = -1e30
QUERY_ROWS = 512
BF16 = jnp.bfloat16
F32 = jnp.float32


def normalize(values):
    factor = lax.rsqrt(jnp.mean(values * values, axis=-1, keepdims=True) + EPSILON)
    return (values * factor, factor)


def contract(left, right, left_dim, right_dim):
    return lax.dot_general(
        left, right, (((left_dim,), (right_dim,)), ((), ())), preferred_element_type=F32
    )


def tie(values, done):
    done = tuple(done)
    if not done:
        return list(values)
    return list(lax.optimization_barrier((tuple(values), done))[0])


class Shares:
    def __init__(self, count):
        self.count = count
        self.index = lax.axis_index("dp")
        self.bits = [1 << i for i in range(count.bit_length() - 1)]
        even = [0]
        for bit in self.bits[1:]:
            even = even + [k ^ bit for k in even]
        self.order = even + [k ^ 1 for k in even] if count > 1 else even

    def swap(self, value, bit):
        return lax.ppermute(value, "dp", [(i, i ^ bit) for i in range(self.count)])

    def relative(self, blocks):
        for bit in self.bits:
            odd = (self.index & bit) != 0
            blocks = [jnp.where(odd, blocks[k ^ bit], blocks[k]) for k in range(self.count)]
        return blocks

    def to_order(self, values):
        blocks = self.relative(jnp.split(values, self.count, axis=1))
        return jnp.concatenate([blocks[k] for k in self.order], axis=1)

    def from_order(self, values):
        parts = jnp.split(values, self.count, axis=1)
        blocks = [parts[self.order.index(k)] for k in range(self.count)]
        return jnp.concatenate(self.relative(blocks), axis=1)

    def gather_far(self, block, done=()):
        (value,) = tie([block], done)
        for bit in self.bits[1:]:
            value = jnp.concatenate([value, self.swap(value, bit)], axis=0)
        return value

    def gather(self, block, done=()):
        value = self.gather_far(block, done)
        return value, self.swap(value, 1)

    def scatter_core(self, kept, given):
        return kept + self.swap(given, 1).astype(F32)

    def scatter_rest(self, total):
        for bit in reversed(self.bits[1:]):
            half = total.shape[0] // 2
            low = total[half:].astype(BF16)
            total = total[:half] + self.swap(low, bit).astype(F32)
        return total.astype(BF16)


class Ring:
    def __init__(self, size):
        self.size = size
        self.order = list(range(0, size, 2)) + list(range(size - 1, 0, -2))
        index = lax.axis_index("ctx")
        self.place = jnp.where(index % 2 == 0, index // 2, size - (index + 1) // 2)
        self.done = ()
        self.steps = []

    def owner(self, ahead):
        place = lax.rem(self.place + ahead, self.size)
        return jnp.where(place < self.size // 2, 2 * place, 2 * (self.size - place) - 1)

    def owners(self):
        return self.owner(jnp.arange(self.size, dtype=jnp.int32))

    def shift(self, value, by):
        pairs = [
            (self.order[i], self.order[(i + by) % self.size]) for i in range(self.size)
        ]
        return lax.ppermute(value, "ctx", pairs)

    def both(self, right, left, done=()):
        right, left = tie((right, left), (*self.done, *done))
        right, left = self.shift(right, 1), self.shift(left, -1)
        self.done = (right, left)
        self.steps.append(self.done)
        return right, left

    def gather(self, value, fill=()):
        size, half = self.size, self.size // 2
        fill = dict(enumerate(fill))
        pieces = [None] * size
        pieces[0] = value
        right = left = value
        for step in range(1, half):
            right, left = self.both(right, left, fill.get(step - 1, ()))
            pieces[size - step] = right
            pieces[step] = left
        rows = value.shape[0] // 2
        pieces[half] = jnp.concatenate(
            self.both(right[:rows], left[rows:], fill.get(half - 1, ())), axis=0
        )
        return pieces

    def scatter_sum(self, lower, upper, fill=()):
        size, half = self.size, self.size // 2
        fill = dict(enumerate(fill))
        rows = lower.shape[0] // size

        def part(ahead, source):
            return source[ahead * rows : (ahead + 1) * rows]

        def whole(ahead):
            return jnp.concatenate([part(ahead, lower), part(ahead, upper)], axis=1)

        right, left = self.both(
            part(half, lower).astype(BF16), part(half, upper).astype(BF16), fill.get(0, ())
        )
        for step in range(1, half):
            if step == 1:
                right = jnp.concatenate(
                    [part(half - 1, lower) + right.astype(F32), part(half - 1, upper)], axis=1
                )
                left = jnp.concatenate(
                    [part(half + 1, lower), part(half + 1, upper) + left.astype(F32)], axis=1
                )
            else:
                right = whole(half - step) + right.astype(F32)
                left = whole(half + step) + left.astype(F32)
            right, left = self.both(
                right.astype(BF16), left.astype(BF16), fill.get(step, ())
            )
        if half == 1:
            return jnp.concatenate(
                [part(0, lower) + right.astype(F32), part(0, upper) + left.astype(F32)], axis=1
            )
        return whole(0) + right.astype(F32) + left.astype(F32)


def column_blocks(weight, size):
    width = weight.shape[1] // size
    return jnp.stack([weight[:, i * width : (i + 1) * width] for i in range(size)])


def join_columns(stacked):
    return jnp.concatenate([stacked[i] for i in range(stacked.shape[0])], axis=1)


def swap_halves(values, half):
    width = values.shape[-1]
    if width == 2 * half:
        return jnp.concatenate([values[:, half:], values[:, :half]], axis=1)
    lane = lax.broadcasted_iota(jnp.int32, values.shape, 1)
    ahead = pltpu.roll(values, width - half, 1)
    behind = pltpu.roll(values, half, 1)
    return jnp.where(lax.rem(lane, 2 * half) < half, ahead, behind)


def head_only(values, lane, head, head_size):
    inside = (lane >= head * head_size) & (lane < (head + 1) * head_size)
    return jnp.where(inside, values, jnp.zeros_like(values))


def flat(ref):
    value = ref[...]
    return value.reshape((value.shape[0] * value.shape[1], value.shape[2]))


def forward_kernel(
    head_size, lengths_ref, q_ref, k_ref, v_ref, cq_ref, sq_ref, ck_ref, sk_ref, qp_ref, kp_ref,
    out_ref, qr_ref, kr_ref, vr_ref, lse_ref,
):
    length = lengths_ref[pl.program_id(0)]
    half = head_size // 2
    queries = flat(q_ref)
    keys = flat(k_ref)
    queries = (queries * cq_ref[...] + swap_halves(queries, half) * sq_ref[...]).astype(BF16)
    keys = (keys * ck_ref[...] + swap_halves(keys, half) * sk_ref[...]).astype(BF16)
    values = flat(v_ref).astype(BF16)
    qr_ref[...] = queries.reshape(qr_ref.shape)
    kr_ref[...] = keys.reshape(kr_ref.shape)
    vr_ref[...] = values.reshape(vr_ref.shape)
    rows, width = queries.shape
    lane = lax.broadcasted_iota(jnp.int32, (rows, width), 1)
    query_pos = qp_ref[:, 0:1]
    key_pos = kp_ref[0:1, :]
    allowed = (key_pos <= query_pos) & (key_pos < length)
    total = jnp.zeros((rows, width), F32)
    scale = head_size ** (-0.5)
    for head in range(width // head_size):
        one = head_only(queries, lane, head, head_size)
        scores = contract(one, keys, 1, 1) * scale
        masked = jnp.where(allowed, scores, NEGATIVE)
        peak = jnp.max(masked, axis=-1, keepdims=True)
        weights = jnp.where(allowed, jnp.exp(masked - peak), 0.0)
        mass = jnp.sum(weights, axis=-1, keepdims=True)
        lse_ref[:, head : head + 1] = peak + jnp.log(mass)
        mixed = contract(weights.astype(BF16), values, 1, 0) / mass
        total = total + head_only(mixed, lane, head, head_size)
    out_ref[...] = total.astype(BF16).reshape(out_ref.shape)


def backward_kernel(
    head_size, lengths_ref, q_ref, k_ref, v_ref, g_ref, lse_ref, cq_ref, sq_ref, ck_ref, sk_ref, qp_ref,
    kp_ref, dq_ref, dk_ref, dv_ref, dk_sum, dv_sum,
):
    length = lengths_ref[pl.program_id(0)]
    half = head_size // 2
    queries, keys, values, grads = flat(q_ref), flat(k_ref), flat(v_ref), flat(g_ref)
    rows, width = queries.shape
    lane = lax.broadcasted_iota(jnp.int32, (rows, width), 1)
    allowed = (kp_ref[0:1, :] <= qp_ref[:, 0:1]) & (kp_ref[0:1, :] < length)
    scale = head_size ** (-0.5)

    @pl.when(pl.program_id(1) == 0)
    def start():
        dk_sum[...] = jnp.zeros_like(dk_sum)
        dv_sum[...] = jnp.zeros_like(dv_sum)

    dq = jnp.zeros((rows, width), F32)
    for head in range(width // head_size):
        one = head_only(queries, lane, head, head_size)
        grad = head_only(grads, lane, head, head_size)
        scores = contract(one, keys, 1, 1) * scale
        prob = jnp.where(
            allowed,
            jnp.exp(jnp.where(allowed, scores, NEGATIVE) - lse_ref[:, head : head + 1]),
            0.0,
        )
        grad_prob = contract(grad, values, 1, 1)
        delta = jnp.sum(prob * grad_prob, axis=-1, keepdims=True)
        grad_score = (prob * (grad_prob - delta) * scale).astype(BF16)
        dq = dq + head_only(contract(grad_score, keys, 1, 0), lane, head, head_size)
        dk_sum[...] += contract(grad_score, one, 0, 0)
        dv_sum[...] += contract(prob.astype(BF16), grad, 0, 0)
    dq = dq * cq_ref[...] - swap_halves(dq, half) * sq_ref[...]
    dq_ref[...] = dq.astype(BF16).reshape(dq_ref.shape)

    @pl.when(pl.program_id(1) == pl.num_programs(1) - 1)
    def finish():
        dk = dk_sum[...]
        dk = dk * ck_ref[...] - swap_halves(dk, half) * sk_ref[...]
        dk_ref[...] = dk.astype(BF16).reshape(dk_ref.shape)
        dv_ref[...] = dv_sum[...].astype(BF16).reshape(dv_ref.shape)


class Attention:
    def __init__(self, size, groups, slots, width, head_size, lengths, owners):
        self.size, self.groups, self.slots, self.width = size, groups, slots, width
        self.head_size = head_size
        self.lengths = lengths
        self.heads = width // head_size
        self.steps = max(1, min(size, QUERY_ROWS // slots))
        half = head_size // 2
        positions = (owners[:, None] * slots + jnp.arange(slots, dtype=jnp.int32)[None]).reshape(-1)
        freqs = THETA ** (-(jnp.arange(half, dtype=F32) * 2.0) / (2.0 * half))
        angles = positions.astype(F32)[:, None] * freqs[None, :]
        cosine, sine = jnp.cos(angles), jnp.sin(angles)
        self.cosine = jnp.tile(cosine, (1, 2 * self.heads))
        self.sine = jnp.tile(jnp.concatenate([-sine, sine], axis=1), (1, self.heads))
        self.query_pos = jnp.broadcast_to(positions[:, None], (positions.shape[0], 128))
        self.key_pos = jnp.broadcast_to(positions[None, :], (8, positions.shape[0]))
        total = size * slots
        rows = self.steps * slots
        self.grid = (groups, size // self.steps)
        self.q_spec = self.tokens(self.steps, width, 0, True)
        self.k_spec = self.tokens(size, width, 0, False)
        self.table_q = pl.BlockSpec((rows, width), lambda b, i, *_: (i, 0))
        self.table_k = pl.BlockSpec((total, width), lambda b, i, *_: (0, 0))
        self.pos_q = pl.BlockSpec((rows, 128), lambda b, i, *_: (i, 0))
        self.pos_k = pl.BlockSpec((8, total), lambda b, i, *_: (0, 0))
        self.lse = pl.BlockSpec((None, rows, self.heads), lambda b, i, *_: (b, i, 0))
        self.lse_shape = jax.ShapeDtypeStruct((groups, total, self.heads), F32)
        self.shape = jax.ShapeDtypeStruct((size, groups, slots, width), BF16)
        self.work = groups * self.heads * total * total

    def tokens(self, count, width, column, moving):
        return pl.BlockSpec(
            (count, None, self.slots, width),
            (lambda b, i, *_: (i, b, 0, column)) if moving else (lambda b, i, *_: (0, b, 0, column)),
        )

    def split(self, array):
        return array.reshape(self.size, self.groups, self.slots, -1)

    def cost(self, matmuls):
        return pl.CostEstimate(
            flops=2 * matmuls * self.work * self.head_size,
            transcendentals=self.work,
            bytes_accessed=8 * self.size * self.groups * self.slots * self.width * 2,
        )

    def forward(self, projected):
        width = self.width
        if width % 128 == 0:
            arrays = (self.split(projected),) * 3
            columns = (0, 1, 2)
        else:
            arrays = tuple(
                self.split(projected[:, i * width : (i + 1) * width]) for i in range(3)
            )
            columns = (0, 0, 0)
        return pl.pallas_call(
            functools.partial(forward_kernel, self.head_size),
            grid_spec=pltpu.PrefetchScalarGridSpec(
                num_scalar_prefetch=1,
                grid=self.grid,
                in_specs=[
                    self.tokens(self.steps, width, columns[0], True),
                    self.tokens(self.size, width, columns[1], False),
                    self.tokens(self.size, width, columns[2], False),
                    self.table_q, self.table_q, self.table_k, self.table_k, self.pos_q, self.pos_k,
                ],
                out_specs=[self.q_spec, self.q_spec, self.k_spec, self.k_spec, self.lse],
            ),
            out_shape=[self.shape] * 4 + [self.lse_shape],
            cost_estimate=self.cost(2),
            name="attention_forward",
        )(
            self.lengths, *arrays, self.cosine, self.sine, self.cosine, self.sine, self.query_pos, self.key_pos
        )

    def backward(self, queries, keys, values, grads, lse):
        total = self.size * self.slots
        return pl.pallas_call(
            functools.partial(backward_kernel, self.head_size),
            grid_spec=pltpu.PrefetchScalarGridSpec(
                num_scalar_prefetch=1,
                grid=self.grid,
                in_specs=[
                    self.q_spec, self.k_spec, self.k_spec, self.q_spec, self.lse,
                    self.table_q, self.table_q, self.table_k, self.table_k, self.pos_q, self.pos_k,
                ],
                out_specs=[self.q_spec, self.k_spec, self.k_spec],
                scratch_shapes=[pltpu.VMEM((total, self.width), F32)] * 2,
            ),
            out_shape=[self.shape] * 3,
            cost_estimate=self.cost(5),
            name="attention_backward",
        )(
            self.lengths, queries, keys, values, self.split(grads), lse,
            self.cosine, self.sine, self.cosine, self.sine, self.query_pos, self.key_pos,
        )


def body(
    inputs, cotangent, lengths, query_weight, key_weight, value_weight, mix_weight, gate_weight,
    up_weight, down_weight, attn_gain, ffn_gain,
):
    groups, slots, width = inputs.shape
    head_size = width // HEADS
    size = lax.axis_size("ctx")
    count = lax.axis_size("dp")
    rows = groups * slots
    ring = Ring(size)
    shares = Shares(count)
    owners = ring.owners()
    local = width // size
    hidden_local = gate_weight.shape[1] // size
    gain_one = attn_gain.astype(F32)[:, None]
    gain_two = ffn_gain.astype(F32)[:, None]

    def scaled(weight, gain):
        return (weight.astype(F32) * gain).astype(BF16)

    def exchange(blocks, done=()):
        return lax.all_to_all(tie([blocks], done)[0], "ctx", 0, 0, tiled=True)

    def to_columns(weights, done=()):
        blocks = jnp.concatenate([column_blocks(w, size) for w in weights], axis=2)
        return exchange(blocks, done).reshape(-1, blocks.shape[2])

    def to_rows(total, done=()):
        return exchange(total.reshape(size, -1, total.shape[1]), done)

    def halves(pieces):
        half = width // 2
        return (
            jnp.concatenate([p[:, :half] for p in pieces], axis=0),
            jnp.concatenate([p[:, half:] for p in pieces], axis=0),
        )

    def apply(values, weights):
        return contract(values[0], weights[0], 1, 0) + contract(values[1], weights[1], 1, 0)

    block_in = shares.to_order(inputs.reshape(rows, width)).astype(F32)
    positions = lax.axis_index("ctx") * slots + jnp.arange(slots, dtype=jnp.int32)
    valid = (positions[None, :] < lengths[:, None]).astype(F32).reshape(rows, 1)
    normed_one, factor_one = normalize(block_in)
    grad_out = shares.to_order(cotangent.reshape(rows, width)).astype(F32) * valid

    to_shares = [(i * size + j, j * count + i) for i in range(count) for j in range(size)]
    from_shares = [(there, here) for here, there in to_shares]
    attn_columns = to_columns([scaled(w, gain_one) for w in (query_weight, key_weight, value_weight)])
    one_all = halves(ring.gather(normed_one.astype(BF16)))
    mix_share = lax.ppermute(tie([mix_weight], ring.steps[-2])[0], ("dp", "ctx"), from_shares)
    attn_weights = shares.gather(attn_columns)
    projected = apply(one_all, attn_weights)
    ffn_columns = to_columns(
        [scaled(gate_weight, gain_two), scaled(up_weight, gain_two), down_weight], ring.done
    )
    ffn_parts = []
    for part in jnp.split(ffn_columns, 6, axis=1):
        ffn_parts.append(shares.gather_far(part, ffn_parts[-1:]))
    ffn_half = jnp.concatenate(ffn_parts[:4], axis=1)
    down_half = jnp.concatenate(ffn_parts[4:], axis=1)
    attention = Attention(size, groups, slots, local, head_size, lengths, owners)
    mixed, query_rot, key_rot, value_low, lse = attention.forward(projected)
    mixed = mixed.reshape(size * rows, local)
    mix_parts = shares.gather(mix_share, (mixed,))
    mix_blocks = jnp.split(jnp.concatenate(mix_parts, axis=0), count, axis=0)
    mix_rows = shares.to_order(
        jnp.concatenate(
            shares.relative([mix_blocks[shares.order.index(k)] for k in range(count)]), axis=0
        )
    )
    attn_out = contract(mixed, mix_rows, 1, 0)
    residual = block_in + ring.scatter_sum(
        attn_out[:, : width // 2], attn_out[:, width // 2 :], ((), (ffn_columns,), ffn_parts[:1], ffn_parts[1:2])
    )

    ffn_weights = (ffn_half, shares.swap(ffn_half, 1))
    normed_two, factor_two = normalize(residual)
    two_all = halves(ring.gather(normed_two.astype(BF16), [(part,) for part in ffn_parts[2:]]))
    down_weights = (down_half, shares.swap(down_half, 1))
    low_part = contract(two_all[0], ffn_weights[0], 1, 0)
    gate_up = low_part + contract(two_all[1], ffn_weights[1], 1, 0)
    gate, up = gate_up[:, :hidden_local], gate_up[:, hidden_local:]
    sigma = jax.nn.sigmoid(gate)
    silu_gate = gate * sigma
    hidden = (silu_gate * up).astype(BF16)
    grad_all = halves(
        ring.gather(grad_out.astype(BF16), fill=((), (low_part,), (gate_up,), (hidden,)))
    )
    branch = ring.scatter_sum(*(contract(hidden, w, 1, 1) for w in down_weights))
    activations = valid * (residual + branch)

    grad_hidden = apply(grad_all, down_weights)
    grad_both = jnp.concatenate(
        [
            (grad_hidden * up * sigma * (1.0 + gate * (1.0 - sigma))).astype(BF16),
            (grad_hidden * silu_gate).astype(BF16),
        ],
        axis=1,
    )

    def summed(values, gradient):
        given = contract(values[1], gradient, 0, 0).astype(BF16)
        return given, shares.scatter_core(contract(values[0], gradient, 0, 0), given)

    down_given, down_half = summed(grad_all, hidden)
    both_given, both_half = summed(two_all, grad_both)
    down_sum = shares.scatter_rest(down_half)
    both_sum = shares.scatter_rest(tie([both_half], (down_sum,))[0])
    scaled_two = ring.scatter_sum(
        *(contract(grad_both, w, 1, 1) for w in ffn_weights),
        fill=((), (down_given,), (both_given,), (down_half,)),
    )
    dres = grad_out + factor_two * (
        scaled_two - normed_two * jnp.mean(normed_two * scaled_two, axis=-1, keepdims=True)
    )
    dres_low = dres.astype(BF16)

    dres_pieces = ring.gather(dres_low, fill=((both_half,),))
    dres_all = jnp.concatenate(dres_pieces, axis=0)
    down_rows = to_rows(down_sum, ring.steps[-2])
    both_rows = to_rows(both_sum, ring.steps[-2])
    grad_heads = contract(dres_all, mix_rows, 1, 1).astype(BF16)
    dq, dk, dv = attention.backward(
        query_rot, key_rot, value_low, *tie([grad_heads], (both_sum, down_rows)), lse
    )
    projected_grad = jnp.concatenate(
        [d.reshape(size * rows, local) for d in (dq, dk, dv)], axis=1
    )
    (projected_grad,) = tie([projected_grad], (both_rows,))
    attn_given, attn_half = summed(one_all, projected_grad)
    attn_sum = shares.scatter_rest(attn_half)
    attn_rows = to_rows(attn_sum)
    mix_terms = shares.from_order(contract(mixed, dres_all, 0, 0))
    mix_blocks = shares.relative(jnp.split(mix_terms, count, axis=0))
    mix_blocks = [mix_blocks[k] for k in shares.order]
    mix_given = jnp.concatenate(mix_blocks[count // 2 :], axis=0).astype(BF16)
    mix_sum = shares.scatter_rest(
        shares.scatter_core(jnp.concatenate(mix_blocks[: count // 2], axis=0), mix_given)
    )
    scaled_one = ring.scatter_sum(
        *(contract(projected_grad, w, 1, 1) for w in attn_weights),
        fill=((attn_given,), (attn_half,), (), (attn_sum,)),
    )
    input_grad = dres + factor_one * (
        scaled_one - normed_one * jnp.mean(normed_one * scaled_one, axis=-1, keepdims=True)
    )
    (mix_sum,) = tie([mix_sum], ring.steps[-2])
    mix_grad = lax.ppermute(mix_sum, ("dp", "ctx"), to_shares).astype(F32)

    def joined(rows, columns):
        return join_columns(rows[:, :, columns]).astype(F32)

    down_grad = joined(down_rows, slice(None))
    gate_raw = joined(both_rows, slice(0, hidden_local))
    up_raw = joined(both_rows, slice(hidden_local, 2 * hidden_local))
    query_raw, key_raw, value_raw = (
        joined(attn_rows, slice(i * local, (i + 1) * local)) for i in range(3)
    )

    def row_sum(*pairs):
        return sum(jnp.sum(w.astype(F32) * g, axis=1) for w, g in pairs)

    attn_gain_grad = row_sum(
        (query_weight, query_raw), (key_weight, key_raw), (value_weight, value_raw)
    )
    ffn_gain_grad = row_sum((gate_weight, gate_raw), (up_weight, up_raw))
    return (
        shares.from_order(activations.astype(BF16)).reshape(groups, slots, width),
        shares.from_order(input_grad.astype(BF16)).reshape(groups, slots, width),
        query_raw * gain_one,
        key_raw * gain_one,
        value_raw * gain_one,
        mix_grad,
        gate_raw * gain_two,
        up_raw * gain_two,
        down_grad,
        attn_gain_grad,
        ffn_gain_grad,
    )


def solution(mesh):
    rows = P(("dp", "ctx"), None)
    tokens = P("dp", "ctx", None)
    gains = P(("dp", "ctx"))
    return jax.shard_map(
        body,
        mesh=mesh,
        in_specs=(tokens, tokens, P("dp")) + (rows,) * 7 + (gains, gains),
        out_specs=(tokens, tokens) + (rows,) * 7 + (gains, gains),
        check_vma=False,
    )
```
